512 devices in a mesh: gx: 32 (over z, y_hi), gy: 16 (over y_lo, x, core).
Axes of the slice: x: 4, y: 8 (y_hi: 4, y_lo: 2; y = y_hi * 2 + y_lo), z: 8, core: 2. Of those that a mesh axis runs over, the one named last changes fastest.
Arguments:
- scalars: float32 [20, 256, 256, 128], P(None, 'gx', 'gy'), may hold values from -6 to 6
- velocity: float32 [3, 256, 256, 128], P(None, 'gx', 'gy'), may hold values from -4 to 4
- diffusivity: float32 [256, 256, 128], P('gx', 'gy'), may hold values from 0.05 to 0.6
- burn_list: int32 [32, 16, 64], P('gx', 'gy'), may hold values from 0 to 128, as said below
- w_in: bfloat16 [800, 20], replicated, may hold values from -1.25 to 1.25
- w_mid: bfloat16 [400, 800], replicated, may hold values from -0.21875 to 0.21875
- w_out: bfloat16 [20, 400], replicated, may hold values from -0.3125 to 0.3125
Outputs:
- scalars_out: float32 [20, 256, 256, 128], P(None, 'gx', 'gy')
- velocity_out: float32 [3, 256, 256, 128], P(None, 'gx', 'gy')
The draws below stay inside these ranges and needn't reach their ends.
Inputs may be any that keep to these rules, and one draw needn't show every extreme that they name: `burn_list`: in each device's list the burning columns come first, distinct, and the remaining slots hold 128. A device lists 0 to 64 burning columns; in every group of devices with one gx index one device lists 64 and one lists none, and the group lists exactly 512 together.
All inputs are finite; a program needn't handle non-finite values.
Results may differ from the reference program's by a relative error of at most 0.0023.
Values may be sent and summed in bfloat16 or wider, within the bound.
No kernel may reach another device: no remote copies, remote signals or barrier semaphores. Data moves between devices by JAX's collectives and lax.ppermute only.
A program may use at most 64 MiB of HBM per device.

```python
import math
import jax
import jax.numpy as jnp
from jax import lax

CX = 8
CY = 16
NZ = 128
NS = 20
H1 = 800
H2 = 400
NX = 256
NY = 256
NB = 128
BURN_DEV = 32
MAXB = 64
N_GX = 32
N_GY = 16


def draw_burn_list(key, part):
    first_key, second_key, third_key = jax.random.split(jax.random.fold_in(key, 7), 3)
    half_group = N_GY // 2
    amount = jax.random.randint(first_key, (N_GX, half_group), 0, BURN_DEV + 1).astype(jnp.int32)
    amount = amount.at[:, 0].set(BURN_DEV)
    counts = jnp.concatenate([BURN_DEV + amount, BURN_DEV - amount], axis=1)
    scores = jax.random.randint(second_key, (N_GX, N_GY), 0, 1 << 20).astype(jnp.int32) * N_GY + jnp.arange(N_GY, dtype=jnp.int32)[None, :]
    shuffle = jnp.argsort(scores, axis=1)
    counts = jnp.take_along_axis(counts, shuffle, axis=1)
    col_scores = jax.random.randint(third_key, (N_GX, N_GY, NB), 0, 1 << 16).astype(jnp.int32) * NB + jnp.arange(NB, dtype=jnp.int32)[None, None, :]
    columns = jnp.argsort(col_scores, axis=2)[:, :, :MAXB].astype(jnp.int32)
    active = jnp.arange(MAXB, dtype=jnp.int32)[None, None, :] < counts[:, :, None]
    return jnp.where(active, columns, NB).astype(jnp.int32)


def levels(key, extent, cuts, smallest, top_value):
    def one(axis_at, shards_of):
        steps = jax.random.uniform(jax.random.fold_in(jax.random.fold_in(key, 6), axis_at), (shards_of,), jnp.float32, smallest / len(cuts), top_value / len(cuts))
        return jnp.repeat(jnp.exp(steps), extent[axis_at] // shards_of).reshape((-1,) + (1,) * (len(extent) - axis_at - 1))

    level = one(*cuts[0])
    for cut in cuts[1:]:
        level = level * one(*cut)
    return level


def centred(own_key, dims, scale, limit, cuts=(), kind=jnp.bfloat16):
    array = scale * jax.random.normal(own_key, dims, jnp.float32)
    if cuts:
        array = array * levels(own_key, dims, cuts, -0.22, 0.18)
    return jnp.clip(array, -limit, limit).astype(kind)


def setup_inputs(seed: int = 0) -> dict:
    seeds = jax.random.split(jax.random.key(seed), 8)
    scalars = centred(seeds[0], (NS, NX, NY, NZ), 1.0, 6.0, ((1, 32), (2, 16)), jnp.float32)
    velocity = centred(seeds[1], (3, NX, NY, NZ), 1.0, 4.0, ((1, 32), (2, 16)), jnp.float32)
    diffusivity = jnp.clip(jnp.exp(math.log(0.6) - 2.4849067 * jax.random.uniform(seeds[2], (NX, NY, NZ), jnp.float32) ** levels(seeds[2], (NX, NY, NZ), ((0, 32), (1, 16)), -0.2, 0.2)), 0.05, 0.6)
    burn_list = draw_burn_list(jax.random.fold_in(seeds[7], 71), 0)
    w_in = centred(seeds[4], (H1, NS), NS ** -0.5, 1.25)
    w_mid = centred(seeds[5], (H2, H1), H1 ** -0.5, 0.21875)
    w_out = centred(seeds[6], (NS, H2), H2 ** -0.5, 0.3125)
    return {"scalars": scalars, "velocity": velocity, "diffusivity": diffusivity, "burn_list": burn_list, "w_in": w_in, "w_mid": w_mid, "w_out": w_out}


time_step = 0.25

def hartley_table(length):
    position = jnp.arange(length, dtype=jnp.int32)
    product = position[:, None] * position[None, :] % length
    phase_angle = 2.0 * math.pi / length * product.astype(jnp.float32)
    return (jnp.cos(phase_angle) + jnp.sin(phase_angle)) / math.sqrt(length)

def cosine_table(length):
    position = jnp.arange(length, dtype=jnp.int32)
    product = position[:, None] * (2 * position[None, :] + 1) % (4 * length)
    phase_angle = math.pi / (2 * length) * product.astype(jnp.float32)
    weight = jnp.where(position == 0, math.sqrt(1.0 / length), math.sqrt(2.0 / length)).astype(jnp.float32)
    return weight[:, None] * jnp.cos(phase_angle)

def depth_next(values):
    return jnp.concatenate([values[..., 1:], values[..., -1:]], -1)

def depth_prev(values):
    return jnp.concatenate([values[..., :1], values[..., :-1]], -1)

def transport_rate(values, velocity, diffusivity):
    x_next = jnp.roll(values, -1, 0)
    x_prev = jnp.roll(values, 1, 0)
    y_next = jnp.roll(values, -1, 1)
    y_prev = jnp.roll(values, 1, 1)
    z_next = depth_next(values)
    z_prev = depth_prev(values)
    coefficient = diffusivity
    advection = velocity[0] * (x_next - x_prev) * 0.5 + velocity[1] * (y_next - y_prev) * 0.5 + velocity[2] * (z_next - z_prev) * 0.5
    diffusion = 0.5 * (coefficient + jnp.roll(coefficient, -1, 0)) * (x_next - values) - 0.5 * (coefficient + jnp.roll(coefficient, 1, 0)) * (values - x_prev)
    diffusion = diffusion + 0.5 * (coefficient + jnp.roll(coefficient, -1, 1)) * (y_next - values) - 0.5 * (coefficient + jnp.roll(coefficient, 1, 1)) * (values - y_prev)
    diffusion = diffusion + 0.5 * (coefficient + depth_next(coefficient)) * (z_next - values) - 0.5 * (coefficient + depth_prev(coefficient)) * (values - z_prev)
    return diffusion - advection

def network(blocks, w_in, w_mid, w_out):
    hidden_one = jnp.einsum('hn,bnz->bhz', w_in.astype(jnp.float32), blocks.astype(jnp.float32))
    hidden_one = jax.nn.gelu(hidden_one).astype(jnp.bfloat16)
    hidden_two = jnp.einsum('kh,bhz->bkz', w_mid.astype(jnp.float32), hidden_one.astype(jnp.float32))
    hidden_two = jax.nn.gelu(hidden_two).astype(jnp.bfloat16)
    return jnp.einsum('nk,bkz->bnz', w_out.astype(jnp.float32), hidden_two.astype(jnp.float32))

def reference(scalars, velocity, diffusivity, burn_list, w_in, w_mid, w_out):

    def advance(values):
        section_one = values + time_step * transport_rate(values, velocity, diffusivity)
        return 0.5 * values + 0.5 * (section_one + time_step * transport_rate(section_one, velocity, diffusivity))
    transported = lax.map(advance, scalars)
    blocked = transported.reshape(NS, N_GX, CX, N_GY, CY, NZ).transpose(1, 3, 0, 2, 4, 5).reshape(N_GX * N_GY, NS, CX * CY, NZ)
    listing = burn_list.reshape(N_GX * N_GY, MAXB)

    def react(member):
        values, listed = member
        picked = jnp.take(values, jnp.minimum(listed, CX * CY - 1), axis=1)
        feed = jnp.transpose(picked, (1, 0, 2)).astype(jnp.bfloat16)
        reaction = network(feed, w_in, w_mid, w_out)
        return values.at[:, listed].add(jnp.transpose(reaction, (1, 0, 2)), mode='drop')
    burned = lax.map(react, (blocked, listing))
    scalars_out = burned.reshape(N_GX, N_GY, NS, CX, CY, NZ).transpose(2, 0, 3, 1, 4, 5).reshape(NS, NX, NY, NZ)
    divergence = 0.5 * (jnp.roll(velocity[0], -1, 0) - jnp.roll(velocity[0], 1, 0))
    divergence = divergence + 0.5 * (jnp.roll(velocity[1], -1, 1) - jnp.roll(velocity[1], 1, 1))
    divergence = divergence + 0.5 * (depth_next(velocity[2]) - depth_prev(velocity[2]))
    highest = lax.Precision.HIGHEST
    table_x = hartley_table(NX)
    table_y = hartley_table(NY)
    table_z = cosine_table(NZ)
    spectrum = jnp.einsum('az,xyz->xya', table_z, divergence, precision=highest)
    spectrum = jnp.einsum('by,xyz->xbz', table_y, spectrum, precision=highest)
    spectrum = jnp.einsum('cx,xyz->cyz', table_x, spectrum, precision=highest)
    mode_x = jnp.arange(NX, dtype=jnp.int32)
    mode_y = jnp.arange(NY, dtype=jnp.int32)
    mode_z = jnp.arange(NZ, dtype=jnp.int32)
    eigen_x = 2.0 - 2.0 * jnp.cos(2.0 * math.pi / NX * mode_x.astype(jnp.float32))
    eigen_y = 2.0 - 2.0 * jnp.cos(2.0 * math.pi / NY * mode_y.astype(jnp.float32))
    eigen_z = 2.0 - 2.0 * jnp.cos(math.pi / NZ * mode_z.astype(jnp.float32))
    eigen = eigen_x[:, None, None] + eigen_y[None, :, None] + eigen_z[None, None, :]
    anchor = ((mode_x[:, None, None] == 0) & (mode_y[None, :, None] == 0) & (mode_z[None, None, :] == 0)).astype(jnp.float32)
    solved = -spectrum * (1.0 - anchor) / (eigen + anchor)
    solved = jnp.einsum('cx,xyz->cyz', table_x, solved, precision=highest)
    solved = jnp.einsum('by,xyz->xbz', table_y, solved, precision=highest)
    pressure = jnp.einsum('az,xya->xyz', table_z, solved, precision=highest)
    grad_x = 0.5 * (jnp.roll(pressure, -1, 0) - jnp.roll(pressure, 1, 0))
    grad_y = 0.5 * (jnp.roll(pressure, -1, 1) - jnp.roll(pressure, 1, 1))
    grad_z = 0.5 * (depth_next(pressure) - depth_prev(pressure))
    velocity_out = velocity - jnp.stack([grad_x, grad_y, grad_z])
    return (scalars_out, velocity_out)
```

```python
import math

import jax
import jax.numpy as jnp
import numpy as np
from jax import lax
from jax.experimental import pallas as pl
from jax.experimental.pallas import tpu as pltpu
from jax.sharding import PartitionSpec as P

time_step = 0.25
f32 = jnp.float32
bf16 = jnp.bfloat16


def split_table(table):
    high = np.asarray(table, np.float64).astype(jnp.bfloat16)
    low = (np.asarray(table, np.float64) - high.astype(np.float64)).astype(jnp.bfloat16)
    return high, low


def product(left, right, contract):
    return lax.dot_general(left, right, (contract, ((), ())), preferred_element_type=f32)


def halves(value):
    high = value.astype(bf16)
    return high, (value - high.astype(f32)).astype(bf16)


def right_table(value, table_high, table_low):
    contract = ((1,), (0,))
    high, low = halves(value)
    return (
        product(high, table_high, contract)
        + product(low, table_high, contract)
        + product(high, table_low, contract)
    )


def times(pair, factor):
    real, imag = pair
    c, s = float(np.real(factor)), float(np.imag(factor))
    if abs(s) < 1e-12:
        return (real, imag) if c > 0 else (-real, -imag)
    if abs(c) < 1e-12:
        return (-imag, real) if s > 0 else (imag, -real)
    if abs(abs(c) - abs(s)) < 1e-12:
        size = abs(c)
        sc, ss = (1 if c > 0 else -1), (1 if s > 0 else -1)
        first = real * size
        second = imag * size
        new_real = (first if sc > 0 else -first) - (second if ss > 0 else -second)
        new_imag = (first if ss > 0 else -first) + (second if sc > 0 else -second)
        return new_real, new_imag
    return real * c - imag * s, real * s + imag * c


def complex_dft(values):
    count = len(values)
    if count == 1:
        return values
    even = complex_dft(values[0::2])
    odd = complex_dft(values[1::2])
    half = count // 2
    low, high = [], []
    for k in range(half):
        turned = times(odd[k], np.exp(-2j * np.pi * k / count))
        low.append((even[k][0] + turned[0], even[k][1] + turned[1]))
        high.append((even[k][0] - turned[0], even[k][1] - turned[1]))
    return low + high


def real_dft(values):
    count = len(values)
    if count == 2:
        zero = jnp.zeros_like(values[0])
        return [(values[0] + values[1], zero), (values[0] - values[1], zero)]
    even = real_dft(values[0::2])
    odd = real_dft(values[1::2])
    half = count // 2
    out = [None] * (half + 1)
    for k in range(half // 2 + 1):
        turned = times(odd[k], np.exp(-2j * np.pi * k / count))
        out[half - k] = (even[k][0] - turned[0], turned[1] - even[k][1])
        out[k] = (even[k][0] + turned[0], even[k][1] + turned[1])
    return out


def full_spectrum(values):
    half = real_dft(values)
    count = len(values)
    return [half[k] if k <= count // 2 else (half[count - k][0], -half[count - k][1]) for k in range(count)]


def turn(pair, cosine, sine):
    real, imag = pair
    return real * cosine + imag * sine, imag * cosine - real * sine


def lane_index(shape):
    return lax.broadcasted_iota(jnp.int32, shape, len(shape) - 1)


def central(values, step, roll):
    count = len(values)
    lane = lane_index(values[0].shape)
    if step == 16:
        digit, top, back = lane // 16, 7, -16
        forward_from_other, backward_from_other = -16, 16
    else:
        digit, top = lane % 16, 15
        forward_from_other, backward_from_other = 15, -15
    last, first = digit == top, digit == 0
    up = [roll(v, -step) for v in values]
    down = [roll(v, step) for v in values]
    up_other = up if step == 16 else [roll(v, forward_from_other) for v in values]
    down_other = down if step == 16 else [roll(v, backward_from_other) for v in values]
    out = []
    for n in range(count):
        after = jnp.where(last, up_other[(n + 1) % count], up[n])
        before = jnp.where(first, down_other[(n - 1) % count], down[n])
        out.append(0.5 * (after - before))
    return out


def depth_modes(velocity, tables):
    plain, derived = tables
    fields = []
    for n in range(3):
        table_high, table_low = plain if n < 2 else derived
        high, low = halves(velocity[n])
        contract = ((1,), (1,))
        fields.append(
            product(table_high, high, contract)
            + product(table_high, low, contract)
            + product(table_low, high, contract)
        )
    return [
        jnp.concatenate([f[4 * n : 4 * n + 4] for f in fields], 0) for n in range(32)
    ]


def forward_x(values, turn_cos, turn_sin, table, roll):
    slope = central([v[0:8] for v in values], 16, roll)
    lines = [
        jnp.concatenate([s[0:4] + v[8:12], v[4:8]], 0) for s, v in zip(slope, values)
    ]
    modes = full_spectrum(lines)
    rows = []
    for k, pair in enumerate(modes):
        rows.append(jnp.concatenate(turn(pair, turn_cos[k : k + 1], turn_sin[k : k + 1]), 1))
    return right_table(jnp.concatenate(rows, 0), *table)


def middle_y(values, turn_cos, turn_sin, table, table_back, eigen_xz, eigen_y, roll):
    plain = [jnp.concatenate([v[0:4], v[8:12]], 0) for v in values]
    other = [jnp.concatenate([v[4:8], v[12:16]], 0) for v in values]
    lines = [p + s for p, s in zip(plain, central(other, 1, roll))]
    rows = []
    for k, pair in enumerate(full_spectrum(lines)):
        rows.append(jnp.concatenate(turn(pair, turn_cos[k : k + 1], turn_sin[k : k + 1]), 1))
    modes = right_table(jnp.concatenate(rows, 0), *table)
    scaled = []
    for k in range(16):
        eigen = eigen_xz + eigen_y[k : k + 1]
        mean_mode = eigen == 0.0
        scale = jnp.where(mean_mode, 0.0, (-1.0 / 65536.0) / jnp.where(mean_mode, 1.0, eigen))
        scaled.append(modes[8 * k : 8 * k + 8] * scale)
    back = right_table(jnp.concatenate(scaled, 0), *table_back)
    pairs = []
    for k in range(16):
        row = back[8 * k : 8 * k + 8]
        pairs.append(turn((row[:, :128], row[:, 128:]), turn_cos[k : k + 1], turn_sin[k : k + 1]))
    pressure = [real - imag for real, imag in complex_dft(pairs)]
    slope = central(pressure, 1, roll)
    return [
        jnp.concatenate([p[0:4], s[0:4], p[4:8], s[4:8]], 0) for p, s in zip(pressure, slope)
    ]


def backward_x(modes, turn_cos, turn_sin, table_back, roll):
    back = right_table(modes, *table_back)
    pairs = []
    for k in range(32):
        row = back[8 * k : 8 * k + 8]
        pairs.append(turn((row[:, :128], row[:, 128:]), turn_cos[k : k + 1], turn_sin[k : k + 1]))
    lines = [real - imag for real, imag in complex_dft(pairs)]
    slope = central(lines, 16, roll)
    return [
        jnp.concatenate([s[0:4], v[4:8], v[0:4]], 0) for s, v in zip(slope, lines)
    ]


def depth_back(fields, velocity, tables):
    plain, derived = tables
    out = []
    for n in range(3):
        table_high, table_low = plain if n < 2 else derived
        turned = fields[n].T.astype(bf16)
        contract = ((1,), (0,))
        gradient = product(turned, table_high, contract) + product(turned, table_low, contract)
        out.append(velocity[n] - gradient)
    return out


def cosine_numpy(length):
    position = np.arange(length)
    weight = np.where(position == 0, math.sqrt(1.0 / length), math.sqrt(2.0 / length))
    return weight[:, None] * np.cos(np.pi / (2 * length) * position[:, None] * (2 * position[None, :] + 1))


def make_tables():
    t = {}
    cosine = cosine_numpy(128)
    above = np.concatenate([cosine[:, 1:], cosine[:, -1:]], 1)
    below = np.concatenate([cosine[:, :1], cosine[:, :-1]], 1)
    t["depth"] = split_table(cosine)
    t["depth_back_slope"] = split_table(0.5 * (above - below))
    slope = np.zeros((128, 128))
    for z in range(128):
        slope[z, min(z + 1, 127)] += 0.5
        slope[z, max(z - 1, 0)] -= 0.5
    t["depth_slope"] = split_table(cosine @ slope)

    def digits(points):
        angle = 2 * np.pi / points * np.outer(np.arange(points), np.arange(points))
        return angle

    eight, sixteen = digits(8), digits(16)
    one16, one8 = np.eye(16), np.eye(8)
    t["x"] = split_table(
        np.concatenate(
            [np.kron(np.cos(eight) + np.sin(eight), one16), np.kron(np.sin(eight) - np.cos(eight), one16)], 0
        )
    )
    t["y"] = split_table(
        np.concatenate(
            [np.kron(one8, np.cos(sixteen) + np.sin(sixteen)), np.kron(one8, np.sin(sixteen) - np.cos(sixteen))], 0
        )
    )
    t["x_back"] = split_table(
        np.concatenate([np.kron(np.cos(eight), one16), np.kron(-np.sin(eight), one16)], 1)
    )
    t["y_back"] = split_table(
        np.concatenate([np.kron(one8, np.cos(sixteen)), np.kron(one8, -np.sin(sixteen))], 1)
    )
    lane = np.arange(128)
    turn_x = 2 * np.pi / 256 * np.outer(np.arange(32), lane // 16)
    turn_y = 2 * np.pi / 256 * np.outer(np.arange(16), lane % 16)
    t["turn_x"] = (np.cos(turn_x).astype(np.float32), np.sin(turn_x).astype(np.float32))
    t["turn_y"] = (np.cos(turn_y).astype(np.float32), np.sin(turn_y).astype(np.float32))
    k1 = np.arange(32)
    eigen_x = 2 - 2 * np.cos(2 * np.pi / 256 * (k1[:, None] + 32 * (lane // 16)[None, :]))
    t["eigen_x"] = np.repeat(eigen_x.reshape(16, 2, 128), 4, axis=1).astype(np.float32)
    kz = 2 - 2 * np.cos(np.pi * np.arange(128) / 128)
    t["eigen_z"] = np.ascontiguousarray(
        np.broadcast_to(np.tile(kz.reshape(32, 4), (1, 2))[:, :, None], (32, 8, 128))
    ).astype(np.float32)
    t["eigen_y"] = (
        2 - 2 * np.cos(2 * np.pi / 256 * (np.arange(16)[:, None] + 16 * (lane % 16)[None, :]))
    ).astype(np.float32)
    return t


def whole(shape):
    return pl.BlockSpec(shape, lambda *_: (0,) * len(shape))


def lane_roll(value, shift):
    return pltpu.roll(value, shift % 128, 1)


def call(body, out_shape, operands, name, limit=16):
    return pl.pallas_call(
        body,
        out_shape=out_shape,
        compiler_params=pltpu.CompilerParams(vmem_limit_bytes=limit << 20),
        name=name,
    )(*operands)


def depth_kernel(velocity, th, tl, sh, sl, out):
    values = [velocity[n] for n in range(3)]
    groups = depth_modes(values, ((th[...], tl[...]), (sh[...], sl[...])))
    for n, group in enumerate(groups):
        out[n] = group.astype(bf16)


def forward_kernel(values, tc, ts, th, tl, out):
    modes = forward_x(
        [values[n].astype(f32) for n in range(32)], tc[...], ts[...], (th[...], tl[...]), lane_roll
    )
    out[...] = modes.reshape(16, 16, 128)


def middle_kernel(place, values, tc, ts, th, tl, bh, bl, ex, ez, ey, out):
    result = middle_y(
        [values[n] for n in range(16)],
        tc[...],
        ts[...],
        (th[...], tl[...]),
        (bh[...], bl[...]),
        ex[place[1]] + ez[place[0]],
        ey[...],
        lane_roll,
    )
    for n, value in enumerate(result):
        out[n] = value


def backward_kernel(values, tc, ts, bh, bl, out):
    result = backward_x(values[...].reshape(256, 128), tc[...], ts[...], (bh[...], bl[...]), lane_roll)
    for n, value in enumerate(result):
        out[n] = value.astype(bf16)


def last_kernel(values, velocity, th, tl, sh, sl, out):
    loaded = [values[n].astype(f32) for n in range(32)]
    fields = [jnp.concatenate([v[4 * n : 4 * n + 4] for v in loaded], 0) for n in range(3)]
    result = depth_back(
        fields, [velocity[n] for n in range(3)], ((th[...], tl[...]), (sh[...], sl[...]))
    )
    for n, value in enumerate(result):
        out[n] = value


def project(velocity):
    t = make_tables()
    columns = velocity.reshape(3, 128, 128)
    modes = call(
        depth_kernel,
        jax.ShapeDtypeStruct((32, 12, 128), bf16),
        (columns, *t["depth"], *t["depth_slope"]),
        "depth_modes",
    )
    modes = lax.all_to_all(modes, "gx", split_axis=0, concat_axis=0, tiled=True)
    modes = call(
        forward_kernel,
        jax.ShapeDtypeStruct((16, 16, 128), f32),
        (modes, *t["turn_x"], *t["x"]),
        "forward_x",
    )
    modes = lax.all_to_all(modes, "gy", split_axis=0, concat_axis=0, tiled=True)
    place = jnp.stack([lax.axis_index("gx"), lax.axis_index("gy")]).astype(jnp.int32)
    modes = pl.pallas_call(
        middle_kernel,
        out_shape=jax.ShapeDtypeStruct((16, 16, 128), f32),
        in_specs=[pl.BlockSpec(memory_space=pltpu.SMEM)] + [pl.BlockSpec(memory_space=pltpu.VMEM)] * 10,
        compiler_params=pltpu.CompilerParams(vmem_limit_bytes=16 << 20),
        name="middle_y",
    )(place, modes, *t["turn_y"], *t["y"], *t["y_back"], t["eigen_x"], t["eigen_z"], t["eigen_y"])
    modes = lax.all_to_all(modes, "gy", split_axis=0, concat_axis=0, tiled=True)
    modes = call(
        backward_kernel,
        jax.ShapeDtypeStruct((32, 12, 128), bf16),
        (modes, *t["turn_x"], *t["x_back"]),
        "backward_x",
    )
    modes = lax.all_to_all(modes, "gx", split_axis=0, concat_axis=0, tiled=True)
    result = call(
        last_kernel,
        jax.ShapeDtypeStruct((3, 128, 128), f32),
        (modes, columns, *t["depth"], *t["depth_back_slope"]),
        "depth_back",
    )
    return result.reshape(velocity.shape)


def padded_2(value, sides, width):
    edges = {}
    for axis, dim in sides:
        size, length = (lax.axis_size(axis), value.shape[dim])
        up = [(i, (i + 1) % size) for i in range(size)]
        last = lax.slice_in_dim(value, length - width, length, axis=dim)
        initial = lax.slice_in_dim(value, 0, width, axis=dim)
        edges[dim] = (
            lax.ppermute(last.astype(bf16), axis, up).astype(value.dtype),
            lax.ppermute(initial.astype(bf16), axis, [(b, a) for a, b in up]).astype(value.dtype),
        )
    done = []
    for _, dim in sides:
        low, high = edges[dim]
        around = [(width, width) if d in done else (0, 0) for d in range(value.ndim)]
        value = jnp.concatenate([jnp.pad(low, around), value, jnp.pad(high, around)], axis=dim)
        done.append(dim)
    return value


def depth_next(values):
    return jnp.concatenate([values[..., 1:], values[..., -1:]], -1)


def depth_prev(values):
    return jnp.concatenate([values[..., :1], values[..., :-1]], -1)


def transport_rate(field_pad, flow_pad):
    center = field_pad[:, 1:-1, 1:-1]
    x_next = field_pad[:, 2:, 1:-1]
    x_prev = field_pad[:, :-2, 1:-1]
    y_next = field_pad[:, 1:-1, 2:]
    y_prev = field_pad[:, 1:-1, :-2]
    z_next = depth_next(center)
    z_prev = depth_prev(center)
    coefficient = flow_pad[3, 1:-1, 1:-1]
    advection = (
        flow_pad[0, 1:-1, 1:-1] * (x_next - x_prev) * 0.5
        + flow_pad[1, 1:-1, 1:-1] * (y_next - y_prev) * 0.5
        + flow_pad[2, 1:-1, 1:-1] * (z_next - z_prev) * 0.5
    )
    diffusion = 0.5 * (coefficient + flow_pad[3, 2:, 1:-1]) * (x_next - center) - 0.5 * (
        coefficient + flow_pad[3, :-2, 1:-1]
    ) * (center - x_prev)
    diffusion = (
        diffusion
        + 0.5 * (coefficient + flow_pad[3, 1:-1, 2:]) * (y_next - center)
        - 0.5 * (coefficient + flow_pad[3, 1:-1, :-2]) * (center - y_prev)
    )
    diffusion = (
        diffusion
        + 0.5 * (coefficient + depth_next(coefficient)) * (z_next - center)
        - 0.5 * (coefficient + depth_prev(coefficient)) * (center - z_prev)
    )
    return diffusion - advection


def network(blocks, w_in, w_mid, w_out):
    block_count = blocks.shape[0]
    bundle_size = 8
    padded_count = -(-block_count // bundle_size) * bundle_size

    def evaluate(bundle):
        hidden_one = jnp.einsum("hn,bnz->bhz", w_in, bundle, preferred_element_type=jnp.float32)
        hidden_one = jax.nn.gelu(hidden_one).astype(jnp.bfloat16)
        hidden_two = jnp.einsum(
            "kh,bhz->bkz", w_mid, hidden_one, preferred_element_type=jnp.float32
        )
        hidden_two = jax.nn.gelu(hidden_two).astype(jnp.bfloat16)
        return jnp.einsum("nk,bkz->bnz", w_out, hidden_two, preferred_element_type=jnp.float32)

    reaction = lax.map(
        evaluate, blocks.reshape((padded_count // bundle_size, bundle_size) + blocks.shape[1:])
    )
    return reaction.reshape((padded_count,) + reaction.shape[2:])


def shards(scalars, velocity, diffusivity, burn_list, w_in, w_mid, w_out):
    channels = scalars.shape[0]
    joined = jnp.concatenate([scalars, diffusivity[None]], 0)
    padded = padded_2(joined, (("gx", 1), ("gy", 2)), 1)
    field_pad = padded[:channels]
    around = ((0, 0), (1, 1), (1, 1), (0, 0))
    inner_flow = jnp.concatenate([jnp.pad(velocity, around), padded[channels:]], 0)
    section_one = scalars + time_step * transport_rate(field_pad, inner_flow)
    section_pad = padded_2(section_one, (("gx", 1), ("gy", 2)), 1)
    transported = 0.5 * scalars + 0.5 * (
        section_one + time_step * transport_rate(section_pad, inner_flow)
    )
    velocity_out = project(velocity)
    cells_x, cells_y, depth = scalars.shape[1:]
    block_total = cells_x * cells_y
    flat_blocks = transported.reshape(channels, block_total, depth)
    listed = burn_list.reshape(-1)
    picked = jnp.take(flat_blocks, jnp.minimum(listed, block_total - 1), axis=1)
    chosen = jnp.transpose(picked, (1, 0, 2)).astype(jnp.bfloat16)
    own_rates = network(chosen, w_in, w_mid, w_out)
    updated = flat_blocks.at[:, listed].add(jnp.transpose(own_rates, (1, 0, 2)), mode="drop")
    scalars_out = updated.reshape(transported.shape)
    return (scalars_out, velocity_out)


def solution(mesh):
    in_specs = (
        P(None, "gx", "gy", None),
        P(None, "gx", "gy", None),
        P("gx", "gy", None),
        P("gx", "gy", None),
        P(),
        P(),
        P(),
    )
    out_specs = (P(None, "gx", "gy", None), P(None, "gx", "gy", None))
    return jax.shard_map(shards, mesh=mesh, in_specs=in_specs, out_specs=out_specs, check_vma=False)
```

```python
import functools
import math

import jax
import jax.numpy as jnp
import numpy as np
from jax import lax
from jax.experimental import pallas as pl
from jax.experimental.pallas import tpu as pltpu
from jax.sharding import PartitionSpec as P


time_step = 0.25
early_slots = 16
f32 = jnp.float32
bf16 = jnp.bfloat16


def split_table(table):
    high = np.asarray(table, np.float64).astype(jnp.bfloat16)
    low = (np.asarray(table, np.float64) - high.astype(np.float64)).astype(jnp.bfloat16)
    return high, low


def product(left, right, contract):
    return lax.dot_general(left, right, (contract, ((), ())), preferred_element_type=f32)


def halves(value):
    high = value.astype(bf16)
    return high, (value - high.astype(f32)).astype(bf16)


def right_table(value, table_high, table_low):
    contract = ((1,), (0,))
    high, low = halves(value)
    return (
        product(high, table_high, contract)
        + product(low, table_high, contract)
        + product(high, table_low, contract)
    )


def times(pair, factor):
    real, imag = pair
    c, s = float(np.real(factor)), float(np.imag(factor))
    if abs(s) < 1e-12:
        return (real, imag) if c > 0 else (-real, -imag)
    if abs(c) < 1e-12:
        return (-imag, real) if s > 0 else (imag, -real)
    if abs(abs(c) - abs(s)) < 1e-12:
        size = abs(c)
        sc, ss = (1 if c > 0 else -1), (1 if s > 0 else -1)
        first = real * size
        second = imag * size
        new_real = (first if sc > 0 else -first) - (second if ss > 0 else -second)
        new_imag = (first if ss > 0 else -first) + (second if sc > 0 else -second)
        return new_real, new_imag
    return real * c - imag * s, real * s + imag * c


def complex_dft(values):
    count = len(values)
    if count == 1:
        return values
    even = complex_dft(values[0::2])
    odd = complex_dft(values[1::2])
    half = count // 2
    low, high = [], []
    for k in range(half):
        turned = times(odd[k], np.exp(-2j * np.pi * k / count))
        low.append((even[k][0] + turned[0], even[k][1] + turned[1]))
        high.append((even[k][0] - turned[0], even[k][1] - turned[1]))
    return low + high


def real_dft(values):
    count = len(values)
    if count == 2:
        zero = jnp.zeros_like(values[0])
        return [(values[0] + values[1], zero), (values[0] - values[1], zero)]
    even = real_dft(values[0::2])
    odd = real_dft(values[1::2])
    half = count // 2
    out = [None] * (half + 1)
    for k in range(half // 2 + 1):
        turned = times(odd[k], np.exp(-2j * np.pi * k / count))
        out[half - k] = (even[k][0] - turned[0], turned[1] - even[k][1])
        out[k] = (even[k][0] + turned[0], even[k][1] + turned[1])
    return out


def full_spectrum(values):
    half = real_dft(values)
    count = len(values)
    return [half[k] if k <= count // 2 else (half[count - k][0], -half[count - k][1]) for k in range(count)]


def turn(pair, cosine, sine):
    real, imag = pair
    return real * cosine + imag * sine, imag * cosine - real * sine


def lane_index(shape):
    return lax.broadcasted_iota(jnp.int32, shape, len(shape) - 1)


def central(values, step, roll):
    count = len(values)
    lane = lane_index(values[0].shape)
    if step == 16:
        digit, top = lane // 16, 7
        forward_from_other, backward_from_other = -16, 16
    else:
        digit, top = lane % 16, 15
        forward_from_other, backward_from_other = 15, -15
    last, first = digit == top, digit == 0
    up = [roll(v, -step) for v in values]
    down = [roll(v, step) for v in values]
    up_other = up if step == 16 else [roll(v, forward_from_other) for v in values]
    down_other = down if step == 16 else [roll(v, backward_from_other) for v in values]
    out = []
    for n in range(count):
        after = jnp.where(last, up_other[(n + 1) % count], up[n])
        before = jnp.where(first, down_other[(n - 1) % count], down[n])
        out.append(0.5 * (after - before))
    return out


def depth_modes(velocity, tables):
    plain, derived = tables
    fields = []
    for n in range(3):
        table_high, table_low = plain if n < 2 else derived
        high, low = halves(velocity[n])
        contract = ((1,), (1,))
        fields.append(
            product(table_high, high, contract)
            + product(table_high, low, contract)
            + product(table_low, high, contract)
        )
    return [
        jnp.concatenate([f[4 * n : 4 * n + 4] for f in fields], 0) for n in range(32)
    ]


def forward_x(values, turn_cos, turn_sin, roll):
    slope = central([v[0:8] for v in values], 16, roll)
    lines = [
        jnp.concatenate([s[0:4] + v[8:12], v[4:8]], 0) for s, v in zip(slope, values)
    ]
    modes = full_spectrum(lines)
    rows = []
    for k, pair in enumerate(modes):
        rows.append(jnp.concatenate(turn(pair, turn_cos[k : k + 1], turn_sin[k : k + 1]), 1))
    return jnp.concatenate(rows, 0)


def middle_y(values, fetch, roll):
    plain = [jnp.concatenate([v[0:4], v[8:12]], 0) for v in values]
    other = [jnp.concatenate([v[4:8], v[12:16]], 0) for v in values]
    lines = [p + s for p, s in zip(plain, central(other, 1, roll))]
    rows = []
    turns = fetch.get("turn")
    turn_cos, turn_sin, eigen_y = turns[:16], turns[16:32], turns[32:48]
    for k, pair in enumerate(full_spectrum(lines)):
        rows.append(jnp.concatenate(turn(pair, turn_cos[k : k + 1], turn_sin[k : k + 1]), 1))
    modes = right_table(jnp.concatenate(rows, 0), *split_pair(fetch.get("y")))
    eigen_xz = fetch.get("ex") + fetch.get("ez")
    scaled = []
    for k in range(16):
        eigen = eigen_xz + eigen_y[k : k + 1]
        mean_mode = eigen == 0.0
        scale = jnp.where(mean_mode, 0.0, (-1.0 / 65536.0) / jnp.where(mean_mode, 1.0, eigen))
        scaled.append(modes[8 * k : 8 * k + 8] * scale)
    back = right_table(jnp.concatenate(scaled, 0), *split_doubled(fetch.get("y_back")))
    pairs = []
    for k in range(16):
        row = back[8 * k : 8 * k + 8]
        pairs.append(turn((row[:, :128], row[:, 128:]), turn_cos[k : k + 1], turn_sin[k : k + 1]))
    pressure = [real - imag for real, imag in complex_dft(pairs)]
    slope = central(pressure, 1, roll)
    return [
        jnp.concatenate([p[0:4], s[0:4], p[4:8], s[4:8]], 0) for p, s in zip(pressure, slope)
    ]


def backward_x(modes, table_back, turn_cos, turn_sin, roll):
    back = right_table(modes, *table_back)
    pairs = []
    for k in range(32):
        row = back[8 * k : 8 * k + 8]
        pairs.append(turn((row[:, :128], row[:, 128:]), turn_cos[k : k + 1], turn_sin[k : k + 1]))
    lines = [real - imag for real, imag in complex_dft(pairs)]
    slope = central(lines, 16, roll)
    return [
        jnp.concatenate([s[0:4], v[4:8], v[0:4]], 0) for s, v in zip(slope, lines)
    ]


def depth_back(fields, tables):
    plain, derived = tables
    out = []
    for n in range(3):
        table_high, table_low = plain if n < 2 else derived
        turned = fields[n].T.astype(bf16)
        contract = ((1,), (0,))
        out.append(product(turned, table_high, contract) + product(turned, table_low, contract))
    return out


def cosine_numpy(length):
    position = np.arange(length)
    weight = np.where(position == 0, math.sqrt(1.0 / length), math.sqrt(2.0 / length))
    return weight[:, None] * np.cos(np.pi / (2 * length) * position[:, None] * (2 * position[None, :] + 1))


def make_tables():
    t = {}
    cosine = cosine_numpy(128)
    above = np.concatenate([cosine[:, 1:], cosine[:, -1:]], 1)
    below = np.concatenate([cosine[:, :1], cosine[:, :-1]], 1)
    t["depth"] = split_table(cosine)
    t["depth_back_slope"] = split_table(0.5 * (above - below))
    slope = np.zeros((128, 128))
    for z in range(128):
        slope[z, min(z + 1, 127)] += 0.5
        slope[z, max(z - 1, 0)] -= 0.5
    t["depth_slope"] = split_table(cosine @ slope)

    def digits(points):
        angle = 2 * np.pi / points * np.outer(np.arange(points), np.arange(points))
        return angle

    eight, sixteen = digits(8), digits(16)
    one16, one8 = np.eye(16), np.eye(8)
    t["x"] = split_table(
        np.concatenate(
            [np.kron(np.cos(eight) + np.sin(eight), one16), np.kron(np.sin(eight) - np.cos(eight), one16)], 0
        )
    )
    t["y"] = split_table(
        np.concatenate(
            [np.kron(one8, np.cos(sixteen) + np.sin(sixteen)), np.kron(one8, np.sin(sixteen) - np.cos(sixteen))], 0
        )
    )
    t["x_back"] = split_table(
        np.concatenate([np.kron(np.cos(eight), one16), np.kron(-np.sin(eight), one16)], 1)
    )
    t["y_back"] = split_table(
        np.concatenate([np.kron(one8, np.cos(sixteen)), np.kron(one8, -np.sin(sixteen))], 1)
    )
    lane = np.arange(128)
    turn_x = 2 * np.pi / 256 * np.outer(np.arange(32), lane // 16)
    turn_y = 2 * np.pi / 256 * np.outer(np.arange(16), lane % 16)
    t["turn_x"] = (np.cos(turn_x).astype(np.float32), np.sin(turn_x).astype(np.float32))
    t["turn_y"] = (np.cos(turn_y).astype(np.float32), np.sin(turn_y).astype(np.float32))
    k1 = np.arange(32)
    eigen_x = 2 - 2 * np.cos(2 * np.pi / 256 * (k1[:, None] + 32 * (lane // 16)[None, :]))
    t["eigen_x"] = np.repeat(eigen_x.reshape(16, 2, 128), 4, axis=1).astype(np.float32)
    kz = 2 - 2 * np.cos(np.pi * np.arange(128) / 128)
    t["eigen_z"] = np.ascontiguousarray(
        np.broadcast_to(np.tile(kz.reshape(32, 4), (1, 2))[:, :, None], (32, 8, 128))
    ).astype(np.float32)
    t["eigen_y"] = (
        2 - 2 * np.cos(2 * np.pi / 256 * (np.arange(16)[:, None] + 16 * (lane % 16)[None, :]))
    ).astype(np.float32)
    return t


def lane_roll(value, shift):
    return pltpu.roll(value, shift % 128, 1)


def pack_tables():
    t = make_tables()
    places, narrow, wide = {}, [], []
    at = 0
    for name in ("depth", "depth_slope", "depth_back_slope", "x", "y", "x_back", "y_back"):
        for n, table in enumerate(t[name]):
            if table.shape[1] == 256:
                table = np.concatenate([table[:, :128], table[:, 128:]], 0)
            places[name, n] = (at, at + table.shape[0])
            narrow.append(table)
            at += table.shape[0]
    at = 0
    for name in ("turn_x", "turn_y", "eigen_y", "eigen_x", "eigen_z"):
        parts = t[name] if isinstance(t[name], tuple) else (t[name],)
        for n, table in enumerate(parts):
            table = table.reshape(-1, 128)
            places[name, n] = (at, at + table.shape[0])
            wide.append(table)
            at += table.shape[0]
    return places, np.concatenate(narrow, 0), np.concatenate(wide, 0)


table_places, narrow_tables, wide_tables = pack_tables()


class Fetch:
    def __init__(self):
        self.copies = {}

    def start(self, name, source, target, flag):
        copy = pltpu.make_async_copy(source, target, flag)
        copy.start()
        self.copies[name] = (copy, target)

    def get(self, name):
        copy, target = self.copies[name]
        copy.wait()
        return target[...]


def rows_of(source, name, last=None):
    low = table_places[name, 0][0]
    high = max(b for (n, _), (_, b) in table_places.items() if n == (last or name))
    return source.at[pl.ds(low, high - low)]


def split_pair(table):
    half = table.shape[0] // 2
    return table[:half], table[half:]


def split_doubled(table):
    return tuple(jnp.concatenate([half[:128], half[128:]], 1) for half in split_pair(table))


def depth_kernel(velocity, narrow, out, one, flags):
    fetch = Fetch()
    fetch.start("depth", rows_of(narrow, "depth", "depth_slope"), one, flags.at[0])
    plain, derived = split_pair(fetch.get("depth"))
    groups = depth_modes([velocity[n] for n in range(3)], (split_pair(plain), split_pair(derived)))
    for n, group in enumerate(groups):
        out[n] = group.astype(bf16)


def forward_kernel(values, narrow, wide, out, one, two, flags):
    fetch = Fetch()
    fetch.start("turn", rows_of(wide, "turn_x"), two, flags.at[0])
    fetch.start("x", rows_of(narrow, "x"), one, flags.at[1])
    loaded = [values[n].astype(f32) for n in range(32)]
    rows = forward_x(loaded, *split_pair(fetch.get("turn")), lane_roll)
    modes = right_table(rows, *split_pair(fetch.get("x")))
    out[...] = modes.reshape(16, 16, 128)


def middle_kernel(values, narrow, wide, out, one, two, three, ex, ez, flags):
    fetch = Fetch()
    at_x = pl.multiple_of(table_places["eigen_x", 0][0] + 8 * lax.axis_index("gy"), 8)
    at_z = pl.multiple_of(table_places["eigen_z", 0][0] + 8 * lax.axis_index("gx"), 8)
    fetch.start("turn", rows_of(wide, "turn_y", "eigen_y"), three, flags.at[0])
    fetch.start("y", rows_of(narrow, "y"), one, flags.at[1])
    fetch.start("y_back", rows_of(narrow, "y_back"), two, flags.at[2])
    fetch.start("ex", wide.at[pl.ds(at_x, 8)], ex, flags.at[3])
    fetch.start("ez", wide.at[pl.ds(at_z, 8)], ez, flags.at[4])
    result = middle_y([values[n] for n in range(16)], fetch, lane_roll)
    for n, value in enumerate(result):
        out[n] = value


def backward_kernel(values, narrow, wide, out, one, two, flags):
    fetch = Fetch()
    fetch.start("x_back", rows_of(narrow, "x_back"), one, flags.at[0])
    fetch.start("turn", rows_of(wide, "turn_x"), two, flags.at[1])
    result = backward_x(
        values[...].reshape(256, 128),
        split_doubled(fetch.get("x_back")),
        *split_pair(fetch.get("turn")),
        lane_roll,
    )
    for n, value in enumerate(result):
        out[n] = value.astype(bf16)


def last_kernel(values, velocity, narrow, out, one, two, kept, flags):
    fetch = Fetch()
    fetch.start("depth", rows_of(narrow, "depth"), one, flags.at[0])
    fetch.start("slope", rows_of(narrow, "depth_back_slope"), two, flags.at[1])
    fetch.start("velocity", velocity, kept, flags.at[2])
    loaded = [values[n].astype(f32) for n in range(32)]
    fields = [jnp.concatenate([v[4 * n : 4 * n + 4] for v in loaded], 0) for n in range(3)]
    tables = (split_pair(fetch.get("depth")), split_pair(fetch.get("slope")))
    gradient = depth_back(fields, tables)
    velocity_before = fetch.get("velocity")
    for n, value in enumerate(gradient):
        out[n] = velocity_before[n] - value


def swap(modes, axis):
    return lax.all_to_all(modes, axis, split_axis=0, concat_axis=0, tiled=True)


def after(value, *others):
    return lax.optimization_barrier((value, *others))


near, far = pl.BlockSpec(memory_space=pltpu.VMEM), pl.BlockSpec(memory_space=pltpu.HBM)


def in_hbm(value):
    return pltpu.with_memory_space_constraint(value, pltpu.HBM)


def fetching(body, out_shape, operands, specs, rows, extra=()):
    scratch = [pltpu.VMEM((count, 128), kind) for count, kind in rows]
    scratch += list(extra) + [pltpu.SemaphoreType.DMA((len(rows) + len(extra),))]
    return pl.pallas_call(
        body,
        out_shape=out_shape,
        in_specs=specs,
        scratch_shapes=scratch,
        compiler_params=pltpu.CompilerParams(vmem_limit_bytes=16 << 20),
    )(*[in_hbm(value) if spec is far else value for value, spec in zip(operands, specs)])


def to_depth_modes(columns, narrow):
    shape = jax.ShapeDtypeStruct((32, 12, 128), bf16)
    return fetching(depth_kernel, shape, (columns, narrow), [near, far], [(512, bf16)])


def to_x_modes(modes, narrow, wide):
    shape = jax.ShapeDtypeStruct((16, 16, 128), f32)
    rows = [(512, bf16), (64, f32)]
    return fetching(forward_kernel, shape, (modes, narrow, wide), [near, far, far], rows)


def solve_y(modes, narrow, wide):
    shape = jax.ShapeDtypeStruct((16, 16, 128), f32)
    rows = [(512, bf16), (512, bf16), (48, f32), (8, f32), (8, f32)]
    return fetching(middle_kernel, shape, (modes, narrow, wide), [near, far, far], rows)


def from_x_modes(modes, narrow, wide):
    shape = jax.ShapeDtypeStruct((32, 12, 128), bf16)
    rows = [(512, bf16), (64, f32)]
    return fetching(backward_kernel, shape, (modes, narrow, wide), [near, far, far], rows)


def from_depth_modes(modes, columns, narrow):
    shape = jax.ShapeDtypeStruct((3, 128, 128), f32)
    rows = [(256, bf16), (256, bf16)]
    extra = [pltpu.VMEM((3, 128, 128), f32)]
    specs = [near, far, far]
    return fetching(last_kernel, shape, (modes, columns, narrow), specs, rows, extra)


def pack_y_kernel(s_far, v_far, k_far, up, down, v, s, k, flags):
    fetch = Fetch()
    fetch.start("s", s_far, s, flags.at[0])
    fetch.start("v", v_far, v, flags.at[1])
    fetch.start("k", k_far, k, flags.at[2])
    for copy, _ in fetch.copies.values():
        copy.wait()
    for side, near, far in ((up, 15, 14), (down, 0, 1)):
        for n in range(20):
            side[n] = s[pl.ds(n * 128 + near, 8, stride=16), :].astype(bf16)
            side[20 + n] = s[pl.ds(n * 128 + far, 8, stride=16), :].astype(bf16)
        side[40] = k[pl.ds(near, 8, stride=16), :].astype(bf16)
        side[41] = k[pl.ds(far, 8, stride=16), :].astype(bf16)
        for n in range(3):
            side[42 + n] = v[pl.ds(n * 128 + near, 8, stride=16), :].astype(bf16)
            side[45 + n] = jnp.zeros((8, 128), bf16)


def pack_x_kernel(s, v, k, ylow, yhigh, up, down, edge, corner):
    edge[0] = ylow[...].astype(f32).reshape(384, 128)
    edge[1] = yhigh[...].astype(f32).reshape(384, 128)
    for side, near, far in ((up, 7, 6), (down, 0, 1)):
        for n in range(20):
            side[n] = s[n * 128 + near * 16 : n * 128 + near * 16 + 16].astype(bf16)
            side[20 + n] = s[n * 128 + far * 16 : n * 128 + far * 16 + 16].astype(bf16)
        side[40] = k[near * 16 : near * 16 + 16].astype(bf16)
        side[41] = k[far * 16 : far * 16 + 16].astype(bf16)
        for n in range(3):
            side[42 + n] = v[n * 128 + near * 16 : n * 128 + near * 16 + 16].astype(bf16)
        for m in range(2):
            for n in range(20):
                corner[20 * m + n : 20 * m + n + 1] = edge[m, n * 8 + near : n * 8 + near + 1]
            corner[40 + m : 41 + m] = edge[m, 320 + near : 321 + near]
        corner[42:48] = jnp.zeros((6, 128), f32)
        for n in range(3):
            side[45 + n] = corner[16 * n : 16 * n + 16].astype(bf16)


def shifted(value, row, step):
    count = value.shape[0]
    index = lax.broadcasted_iota(jnp.int32, value.shape, 0)
    if step > 0:
        return jnp.where(index == count - 1, row, pltpu.roll(value, count - 1, 0))
    return jnp.where(index == 0, row, pltpu.roll(value, 1, 0))


def weights_of(k, kxn, kxp, kyn, kyp, u, v, w):
    lane = lane_index(k.shape)
    last, first = lane == 127, lane == 0
    kzn = jnp.where(last, k, pltpu.roll(k, 127, 1))
    kzp = jnp.where(first, k, pltpu.roll(k, 1, 1))
    eighth = 0.5 * time_step
    half = 0.5 * eighth * 2.0
    xn, xp = half * (k + kxn - u), half * (k + kxp + u)
    yn, yp = half * (k + kyn - v), half * (k + kyp + v)
    zn, zp = half * (k + kzn - w), half * (k + kzp + w)
    own = 1.0 - half * (6.0 * k + kxn + kxp + kyn + kyp + kzn + kzp)
    own = own + jnp.where(last, zn, 0.0) + jnp.where(first, zp, 0.0)
    return own, xn, xp, yn, yp, jnp.where(last, 0.0, zn), jnp.where(first, 0.0, zp)


def stepped(c, f, xn, xp, yn, yp):
    total = c[0] * f + c[1] * xn + c[2] * xp
    total = total + (c[3] * yn + c[4] * yp)
    return total + (c[5] * pltpu.roll(f, 127, 1) + c[6] * pltpu.roll(f, 1, 1))


def transport_kernel(s_far, v, k, ylow, yhigh, xlow, xhigh, out, s, yf, xf, cx, cy, flags):
    fetch = Fetch()
    fetch.start("s", s_far, s, flags.at[0])
    yf[0] = ylow[...].astype(f32).reshape(384, 128)
    yf[1] = yhigh[...].astype(f32).reshape(384, 128)
    xf[0] = xlow[...].astype(f32).reshape(768, 128)
    xf[1] = xhigh[...].astype(f32).reshape(768, 128)

    def plane(side, n):
        return xf[side, 16 * n : 16 * n + 16]

    def strip(side, n):
        return yf[side, 8 * n : 8 * n + 8]

    ks = [plane(0, 41), plane(0, 40)] + [k[16 * n : 16 * n + 16] for n in range(8)] + [plane(1, 40), plane(1, 41)]
    for p in range(10):
        if p == 0 or p == 9:
            side = 0 if p == 0 else 1
            flow = [plane(side, 42 + n) for n in range(3)]
            row_low, row_high = xf[side, 760:761], xf[side, 761:762]
        else:
            x = p - 1
            flow = [v[n * 128 + 16 * x : n * 128 + 16 * x + 16] for n in range(3)]
            row_low, row_high = yf[0, 320 + x : 321 + x], yf[1, 320 + x : 321 + x]
        own = ks[p + 1]
        made = weights_of(
            own, ks[p + 2], ks[p], shifted(own, row_high, 1), shifted(own, row_low, -1), *flow
        )
        for n in range(7):
            cx[p, n] = made[n]
    for side in range(2):
        own = strip(side, 40)
        inner = k[pl.ds(15 * side, 8, stride=16), :]
        around = (inner, strip(0, 41)) if side == 0 else (strip(1, 41), inner)
        made = weights_of(
            own,
            shifted(own, xf[1, 760 + side : 761 + side], 1),
            shifted(own, xf[0, 760 + side : 761 + side], -1),
            *around,
            *[strip(side, 42 + n) for n in range(3)],
        )
        for n in range(7):
            cy[side, n] = made[n]

    def channel(n, carry):
        base = pl.multiple_of(n * 128, 128)

        def far_plane(side, m):
            return xf[side, pl.ds(pl.multiple_of(m * 16, 16), 16), :]

        def far_strip(side, m):
            return yf[side, pl.ds(pl.multiple_of(m * 8, 8), 8), :]

        fields = [s[pl.ds(base + 16 * x, 16), :] for x in range(8)]
        planes = [far_plane(0, 20 + n), far_plane(0, n)] + fields + [far_plane(1, n), far_plane(1, 20 + n)]
        strips = [far_strip(side, n) for side in range(2)]
        far = [far_strip(side, 20 + n) for side in range(2)]
        corners = [[xf[side, pl.ds(720 + 20 * m + n, 1), :] for m in range(2)] for side in range(2)]
        section = []
        for p in range(10):
            if p == 0 or p == 9:
                row_low, row_high = corners[0 if p == 0 else 1]
            else:
                row_low, row_high = strips[0][p - 1 : p], strips[1][p - 1 : p]
            own = planes[p + 1]
            section.append(
                stepped(
                    [cx[p, m] for m in range(7)],
                    own,
                    planes[p + 2],
                    planes[p],
                    shifted(own, row_high, 1),
                    shifted(own, row_low, -1),
                )
            )
        edges = []
        for side in range(2):
            own = strips[side]
            inner = s[pl.ds(base + 15 * side, 8, stride=16), :]
            around = (inner, far[0]) if side == 0 else (far[1], inner)
            edges.append(
                stepped(
                    [cy[side, m] for m in range(7)],
                    own,
                    shifted(own, corners[1][side], 1),
                    shifted(own, corners[0][side], -1),
                    *around,
                )
            )
        for x in range(8):
            own = section[x + 1]
            moved = stepped(
                [cx[x + 1, m] for m in range(7)],
                own,
                section[x + 2],
                section[x],
                shifted(own, edges[1][x : x + 1], 1),
                shifted(own, edges[0][x : x + 1], -1),
            )
            out[pl.ds(base + 16 * x, 16), :] = 0.5 * (fields[x] + moved)
        return carry

    fetch.copies["s"][0].wait()
    lax.fori_loop(0, 20, channel, 0)


def gelu(x):
    inner = 0.7978845608028654 * (x + 0.044715 * (x * x * x))
    half = 0.5 * x
    return half + half * jnp.tanh(inner)


bundle = 4


def react_kernel(begin, end, listed, s, in_far, mid_far, out_far, out, w_in, w_mid, w_out, raw, flags):
    fetch = Fetch()
    fetch.start("in", in_far, raw, flags.at[0])
    fetch.start("mid", mid_far, w_mid, flags.at[1])
    fetch.start("out", out_far, w_out, flags.at[2])
    out[...] = s[...]
    w_in[...] = fetch.get("in").astype(f32).T.astype(bf16)
    for name in ("mid", "out"):
        fetch.copies[name][0].wait()

    def step(g, carry):
        first = g * bundle

        @pl.when(listed[first] < 128)
        def _():
            places = [listed[first + q] for q in range(bundle)]
            bounded = [jnp.minimum(place, 127) for place in places]
            rows = [s[pl.ds(place, 20, stride=128), :] for place in bounded]
            feed = jnp.concatenate(rows, 1).astype(bf16)
            one = gelu(product(w_in[...], feed, ((1,), (0,)))).astype(bf16)
            two = gelu(product(w_mid[...], one, ((1,), (0,)))).astype(bf16)
            change = product(w_out[...], two, ((1,), (0,)))
            for q in range(bundle):

                @pl.when(places[q] < 128)
                def _():
                    out[pl.ds(bounded[q], 20, stride=128), :] = (
                        rows[q] + change[:, 128 * q : 128 * q + 128]
                    )

        return carry

    lax.fori_loop(begin // bundle, end // bundle, step, 0)


def exchange(up, down, axis):
    size = lax.axis_size(axis)
    forward = [(n, (n + 1) % size) for n in range(size)]
    low = lax.ppermute(up, axis, forward)
    return low, lax.ppermute(down, axis, [(b, a) for a, b in forward])


def pack_y(s, v, k):
    strip = jax.ShapeDtypeStruct((48, 8, 128), bf16)
    return pl.pallas_call(
        pack_y_kernel,
        out_shape=(strip, strip, jax.ShapeDtypeStruct((384, 128), f32)),
        in_specs=[far] * 3,
        out_specs=(near,) * 3,
        scratch_shapes=[
            pltpu.VMEM((2560, 128), f32),
            pltpu.VMEM((128, 128), f32),
            pltpu.SemaphoreType.DMA((3,)),
        ],
        compiler_params=pltpu.CompilerParams(vmem_limit_bytes=16 << 20),
        name="pack_y",
    )(in_hbm(s), in_hbm(v), in_hbm(k))


def pack_x(s, v, k, ylow, yhigh):
    face = jax.ShapeDtypeStruct((48, 16, 128), bf16)
    return pl.pallas_call(
        pack_x_kernel,
        out_shape=(face, face),
        scratch_shapes=[pltpu.VMEM((2, 384, 128), f32), pltpu.VMEM((48, 128), f32)],
        compiler_params=pltpu.CompilerParams(vmem_limit_bytes=16 << 20),
        name="pack_x",
    )(s, v, k, ylow, yhigh)


def transport(s, v, k, strips, faces):
    return pl.pallas_call(
        transport_kernel,
        out_shape=jax.ShapeDtypeStruct((2560, 128), f32),
        in_specs=[far] + [near] * 6,
        scratch_shapes=[
            pltpu.VMEM((2560, 128), f32),
            pltpu.VMEM((2, 384, 128), f32),
            pltpu.VMEM((2, 768, 128), f32),
            pltpu.VMEM((10, 7, 16, 128), f32),
            pltpu.VMEM((2, 7, 8, 128), f32),
            pltpu.SemaphoreType.DMA((1,)),
        ],
        compiler_params=pltpu.CompilerParams(vmem_limit_bytes=24 << 20),
        name="transport",
    )(in_hbm(s), v, k, *strips, *faces)


def react(moved, listed, network, begin, end):
    w_in, w_mid, w_out = network
    return pl.pallas_call(
        functools.partial(react_kernel, begin, end),
        out_shape=jax.ShapeDtypeStruct((2560, 128), f32),
        in_specs=[pl.BlockSpec(memory_space=pltpu.SMEM), near, far, far, far],
        scratch_shapes=[
            pltpu.VMEM((800, 20), bf16),
            pltpu.VMEM((400, 800), bf16),
            pltpu.VMEM((20, 400), bf16),
            pltpu.VMEM((20, 800), bf16),
            pltpu.SemaphoreType.DMA((3,)),
        ],
        compiler_params=pltpu.CompilerParams(vmem_limit_bytes=32 << 20),
        name="react",
    )(listed, moved, in_hbm(w_in.T), in_hbm(w_mid), in_hbm(w_out))


def advance(scalars, velocity, diffusivity, burn_list, w_in, w_mid, w_out):
    s = scalars.reshape(2560, 128)
    v = velocity.reshape(384, 128)
    k = diffusivity.reshape(128, 128)
    listed = burn_list.reshape(64)
    up, down, kept = pack_y(s, v, k)
    narrow, wide = jnp.asarray(narrow_tables), jnp.asarray(wide_tables)
    network = (w_in, w_mid, w_out)
    strips = exchange(up, down, "gy")
    modes = to_depth_modes(kept.reshape(3, 128, 128), narrow)
    modes = swap(modes, "gx")
    up, down = pack_x(s, v, k, *strips)
    faces = exchange(up, down, "gx")
    modes, up, down = after(modes, up, down)
    modes = to_x_modes(modes, narrow, wide)
    modes = swap(modes, "gy")
    moved = transport(s, v, k, strips, faces)
    modes, moved = after(modes, moved)
    modes = swap(solve_y(modes, narrow, wide), "gy")
    moved = react(moved, listed, network, 0, early_slots)
    modes, moved = after(modes, moved)
    modes = swap(from_x_modes(modes, narrow, wide), "gx")
    moved = react(moved, listed, network, early_slots, 64)
    velocity_out = from_depth_modes(modes, velocity.reshape(3, 128, 128), narrow)
    return (moved.reshape(scalars.shape), velocity_out.reshape(velocity.shape))


def solution(mesh):
    in_specs = (
        P(None, "gx", "gy", None),
        P(None, "gx", "gy", None),
        P("gx", "gy", None),
        P("gx", "gy", None),
        P(),
        P(),
        P(),
    )
    out_specs = (P(None, "gx", "gy", None), P(None, "gx", "gy", None))
    return jax.shard_map(advance, mesh=mesh, in_specs=in_specs, out_specs=out_specs, check_vma=False)
```

```python
import functools
import math

import jax
import jax.numpy as jnp
import numpy as np
from jax import lax
from jax.experimental import pallas as pl
from jax.experimental.pallas import tpu as pltpu
from jax.sharding import PartitionSpec as P


time_step = 0.25
early_slots = 16
f32 = jnp.float32
bf16 = jnp.bfloat16


def split_table(table):
    high = np.asarray(table, np.float64).astype(jnp.bfloat16)
    low = (np.asarray(table, np.float64) - high.astype(np.float64)).astype(jnp.bfloat16)
    return high, low


def product(left, right, contract):
    return lax.dot_general(left, right, (contract, ((), ())), preferred_element_type=f32)


def halves(value):
    high = value.astype(bf16)
    return high, (value - high.astype(f32)).astype(bf16)


def right_table(value, table_high, table_low):
    contract = ((1,), (0,))
    high, low = halves(value)
    return (
        product(high, table_high, contract)
        + product(low, table_high, contract)
        + product(high, table_low, contract)
    )


def times(pair, factor):
    real, imag = pair
    c, s = float(np.real(factor)), float(np.imag(factor))
    if abs(s) < 1e-12:
        return (real, imag) if c > 0 else (-real, -imag)
    if abs(c) < 1e-12:
        return (-imag, real) if s > 0 else (imag, -real)
    if abs(abs(c) - abs(s)) < 1e-12:
        size = abs(c)
        sc, ss = (1 if c > 0 else -1), (1 if s > 0 else -1)
        first = real * size
        second = imag * size
        new_real = (first if sc > 0 else -first) - (second if ss > 0 else -second)
        new_imag = (first if ss > 0 else -first) + (second if sc > 0 else -second)
        return new_real, new_imag
    return real * c - imag * s, real * s + imag * c


def complex_dft(values):
    count = len(values)
    if count == 1:
        return values
    even = complex_dft(values[0::2])
    odd = complex_dft(values[1::2])
    half = count // 2
    low, high = [], []
    for k in range(half):
        turned = times(odd[k], np.exp(-2j * np.pi * k / count))
        low.append((even[k][0] + turned[0], even[k][1] + turned[1]))
        high.append((even[k][0] - turned[0], even[k][1] - turned[1]))
    return low + high


def real_dft(values):
    count = len(values)
    if count == 2:
        zero = jnp.zeros_like(values[0])
        return [(values[0] + values[1], zero), (values[0] - values[1], zero)]
    even = real_dft(values[0::2])
    odd = real_dft(values[1::2])
    half = count // 2
    out = [None] * (half + 1)
    for k in range(half // 2 + 1):
        turned = times(odd[k], np.exp(-2j * np.pi * k / count))
        out[half - k] = (even[k][0] - turned[0], turned[1] - even[k][1])
        out[k] = (even[k][0] + turned[0], even[k][1] + turned[1])
    return out


def full_spectrum(values):
    half = real_dft(values)
    count = len(values)
    return [half[k] if k <= count // 2 else (half[count - k][0], -half[count - k][1]) for k in range(count)]


def turn(pair, cosine, sine):
    real, imag = pair
    return real * cosine + imag * sine, imag * cosine - real * sine


def lane_index(shape):
    return lax.broadcasted_iota(jnp.int32, shape, len(shape) - 1)


def central(values, step, roll):
    count = len(values)
    lane = lane_index(values[0].shape)
    if step == 16:
        digit, top = lane // 16, 7
        forward_from_other, backward_from_other = -16, 16
    else:
        digit, top = lane % 16, 15
        forward_from_other, backward_from_other = 15, -15
    last, first = digit == top, digit == 0
    up = [roll(v, -step) for v in values]
    down = [roll(v, step) for v in values]
    up_other = up if step == 16 else [roll(v, forward_from_other) for v in values]
    down_other = down if step == 16 else [roll(v, backward_from_other) for v in values]
    out = []
    for n in range(count):
        after = jnp.where(last, up_other[(n + 1) % count], up[n])
        before = jnp.where(first, down_other[(n - 1) % count], down[n])
        out.append(0.5 * (after - before))
    return out


def depth_modes(velocity, tables):
    plain, derived = tables
    fields = []
    for n in range(3):
        table_high, table_low = plain if n < 2 else derived
        high, low = halves(velocity[n])
        contract = ((1,), (1,))
        fields.append(
            product(table_high, high, contract)
            + product(table_high, low, contract)
            + product(table_low, high, contract)
        )
    return [
        jnp.concatenate([f[4 * n : 4 * n + 4] for f in fields], 0) for n in range(32)
    ]


def forward_x(values, turn_cos, turn_sin, roll):
    slope = central([v[0:8] for v in values], 16, roll)
    lines = [
        jnp.concatenate([s[0:4] + v[8:12], v[4:8]], 0) for s, v in zip(slope, values)
    ]
    modes = full_spectrum(lines)
    rows = []
    for k, pair in enumerate(modes):
        rows.append(jnp.concatenate(turn(pair, turn_cos[k : k + 1], turn_sin[k : k + 1]), 1))
    return jnp.concatenate(rows, 0)


def middle_y(values, fetch, roll):
    plain = [jnp.concatenate([v[0:4], v[8:12]], 0) for v in values]
    other = [jnp.concatenate([v[4:8], v[12:16]], 0) for v in values]
    lines = [p + s for p, s in zip(plain, central(other, 1, roll))]
    rows = []
    turns = fetch.get("turn")
    turn_cos, turn_sin, eigen_y = turns[:16], turns[16:32], turns[32:48]
    for k, pair in enumerate(full_spectrum(lines)):
        rows.append(jnp.concatenate(turn(pair, turn_cos[k : k + 1], turn_sin[k : k + 1]), 1))
    modes = right_table(jnp.concatenate(rows, 0), *split_pair(fetch.get("y")))
    eigen_xz = fetch.get("ex") + fetch.get("ez")
    scaled = []
    for k in range(16):
        eigen = eigen_xz + eigen_y[k : k + 1]
        mean_mode = eigen == 0.0
        scale = jnp.where(mean_mode, 0.0, (-1.0 / 65536.0) / jnp.where(mean_mode, 1.0, eigen))
        scaled.append(modes[8 * k : 8 * k + 8] * scale)
    back = right_table(jnp.concatenate(scaled, 0), *split_doubled(fetch.get("y_back")))
    pairs = []
    for k in range(16):
        row = back[8 * k : 8 * k + 8]
        pairs.append(turn((row[:, :128], row[:, 128:]), turn_cos[k : k + 1], turn_sin[k : k + 1]))
    pressure = [real - imag for real, imag in complex_dft(pairs)]
    slope = central(pressure, 1, roll)
    return [
        jnp.concatenate([p[0:4], s[0:4], p[4:8], s[4:8]], 0) for p, s in zip(pressure, slope)
    ]


def backward_x(modes, table_back, turn_cos, turn_sin, roll):
    back = right_table(modes, *table_back)
    pairs = []
    for k in range(32):
        row = back[8 * k : 8 * k + 8]
        pairs.append(turn((row[:, :128], row[:, 128:]), turn_cos[k : k + 1], turn_sin[k : k + 1]))
    lines = [real - imag for real, imag in complex_dft(pairs)]
    slope = central(lines, 16, roll)
    return [
        jnp.concatenate([s[0:4], v[4:8], v[0:4]], 0) for s, v in zip(slope, lines)
    ]


def depth_back(fields, tables):
    plain, derived = tables
    out = []
    for n in range(3):
        table_high, table_low = plain if n < 2 else derived
        turned = fields[n].T.astype(bf16)
        contract = ((1,), (0,))
        out.append(product(turned, table_high, contract) + product(turned, table_low, contract))
    return out


def cosine_numpy(length):
    position = np.arange(length)
    weight = np.where(position == 0, math.sqrt(1.0 / length), math.sqrt(2.0 / length))
    return weight[:, None] * np.cos(np.pi / (2 * length) * position[:, None] * (2 * position[None, :] + 1))


def make_tables():
    t = {}
    cosine = cosine_numpy(128)
    above = np.concatenate([cosine[:, 1:], cosine[:, -1:]], 1)
    below = np.concatenate([cosine[:, :1], cosine[:, :-1]], 1)
    t["depth"] = split_table(cosine)
    t["depth_back_slope"] = split_table(0.5 * (above - below))
    slope = np.zeros((128, 128))
    for z in range(128):
        slope[z, min(z + 1, 127)] += 0.5
        slope[z, max(z - 1, 0)] -= 0.5
    t["depth_slope"] = split_table(cosine @ slope)

    def digits(points):
        angle = 2 * np.pi / points * np.outer(np.arange(points), np.arange(points))
        return angle

    eight, sixteen = digits(8), digits(16)
    one16, one8 = np.eye(16), np.eye(8)
    t["x"] = split_table(
        np.concatenate(
            [np.kron(np.cos(eight) + np.sin(eight), one16), np.kron(np.sin(eight) - np.cos(eight), one16)], 0
        )
    )
    t["y"] = split_table(
        np.concatenate(
            [np.kron(one8, np.cos(sixteen) + np.sin(sixteen)), np.kron(one8, np.sin(sixteen) - np.cos(sixteen))], 0
        )
    )
    t["x_back"] = split_table(
        np.concatenate([np.kron(np.cos(eight), one16), np.kron(-np.sin(eight), one16)], 1)
    )
    t["y_back"] = split_table(
        np.concatenate([np.kron(one8, np.cos(sixteen)), np.kron(one8, -np.sin(sixteen))], 1)
    )
    lane = np.arange(128)
    turn_x = 2 * np.pi / 256 * np.outer(np.arange(32), lane // 16)
    turn_y = 2 * np.pi / 256 * np.outer(np.arange(16), lane % 16)
    t["turn_x"] = (np.cos(turn_x).astype(np.float32), np.sin(turn_x).astype(np.float32))
    t["turn_y"] = (np.cos(turn_y).astype(np.float32), np.sin(turn_y).astype(np.float32))
    k1 = np.arange(32)
    eigen_x = 2 - 2 * np.cos(2 * np.pi / 256 * (k1[:, None] + 32 * (lane // 16)[None, :]))
    t["eigen_x"] = np.repeat(eigen_x.reshape(16, 2, 128), 4, axis=1).astype(np.float32)
    kz = 2 - 2 * np.cos(np.pi * np.arange(128) / 128)
    t["eigen_z"] = np.ascontiguousarray(
        np.broadcast_to(np.tile(kz.reshape(32, 4), (1, 2))[:, :, None], (32, 8, 128))
    ).astype(np.float32)
    t["eigen_y"] = (
        2 - 2 * np.cos(2 * np.pi / 256 * (np.arange(16)[:, None] + 16 * (lane % 16)[None, :]))
    ).astype(np.float32)
    return t


def lane_roll(value, shift):
    return pltpu.roll(value, shift % 128, 1)


def call(body, out_shape, operands, limit=16):
    return pl.pallas_call(
        body,
        out_shape=out_shape,
        compiler_params=pltpu.CompilerParams(vmem_limit_bytes=limit << 20),
    )(*operands)


def pack_tables():
    t = make_tables()
    places, narrow, wide = {}, [], []
    at = 0
    for name in ("depth", "depth_slope", "depth_back_slope", "x", "y", "x_back", "y_back"):
        for n, table in enumerate(t[name]):
            if table.shape[1] == 256:
                table = np.concatenate([table[:, :128], table[:, 128:]], 0)
            places[name, n] = (at, at + table.shape[0])
            narrow.append(table)
            at += table.shape[0]
    at = 0
    for name in ("turn_x", "turn_y", "eigen_y", "eigen_x", "eigen_z"):
        parts = t[name] if isinstance(t[name], tuple) else (t[name],)
        for n, table in enumerate(parts):
            table = table.reshape(-1, 128)
            places[name, n] = (at, at + table.shape[0])
            wide.append(table)
            at += table.shape[0]
    return places, np.concatenate(narrow, 0), np.concatenate(wide, 0)


table_places, narrow_tables, wide_tables = pack_tables()


class Fetch:
    def __init__(self):
        self.copies = {}

    def start(self, name, source, target, flag):
        copy = pltpu.make_async_copy(source, target, flag)
        copy.start()
        self.copies[name] = (copy, target)

    def get(self, name):
        copy, target = self.copies[name]
        copy.wait()
        return target[...]


def rows_of(source, name, last=None):
    low = table_places[name, 0][0]
    high = max(b for (n, _), (_, b) in table_places.items() if n == (last or name))
    return source.at[pl.ds(low, high - low)]


def split_pair(table):
    half = table.shape[0] // 2
    return table[:half], table[half:]


def split_doubled(table):
    return tuple(jnp.concatenate([half[:128], half[128:]], 1) for half in split_pair(table))


def depth_kernel(velocity, table, out):
    plain, derived = split_pair(table[...])
    groups = depth_modes([velocity[n] for n in range(3)], (split_pair(plain), split_pair(derived)))
    for n, group in enumerate(groups):
        out[n] = group.astype(bf16)


def forward_kernel(values, table, turns, out):
    loaded = [values[n].astype(f32) for n in range(32)]
    rows = forward_x(loaded, *split_pair(turns[...]), lane_roll)
    modes = right_table(rows, *split_pair(table[...]))
    out[...] = modes.reshape(16, 16, 128)


def middle_kernel(values, narrow, wide, out, one, two, three, ex, ez, flags):
    fetch = Fetch()
    at_x = pl.multiple_of(table_places["eigen_x", 0][0] + 8 * lax.axis_index("gy"), 8)
    at_z = pl.multiple_of(table_places["eigen_z", 0][0] + 8 * lax.axis_index("gx"), 8)
    fetch.start("turn", rows_of(wide, "turn_y", "eigen_y"), three, flags.at[0])
    fetch.start("y", rows_of(narrow, "y"), one, flags.at[1])
    fetch.start("y_back", rows_of(narrow, "y_back"), two, flags.at[2])
    fetch.start("ex", wide.at[pl.ds(at_x, 8)], ex, flags.at[3])
    fetch.start("ez", wide.at[pl.ds(at_z, 8)], ez, flags.at[4])
    result = middle_y([values[n] for n in range(16)], fetch, lane_roll)
    for n, value in enumerate(result):
        out[n] = value


def backward_kernel(values, narrow, wide, out, one, two, flags):
    fetch = Fetch()
    fetch.start("x_back", rows_of(narrow, "x_back"), one, flags.at[0])
    fetch.start("turn", rows_of(wide, "turn_x"), two, flags.at[1])
    result = backward_x(
        values[...].reshape(256, 128),
        split_doubled(fetch.get("x_back")),
        *split_pair(fetch.get("turn")),
        lane_roll,
    )
    for n, value in enumerate(result):
        out[n] = value.astype(bf16)


def last_kernel(values, velocity, table, out, kept, flags):
    fetch = Fetch()
    fetch.start("velocity", velocity, kept, flags.at[0])
    loaded = [values[n].astype(f32) for n in range(32)]
    fields = [jnp.concatenate([v[4 * n : 4 * n + 4] for v in loaded], 0) for n in range(3)]
    plain, derived = split_pair(table[...])
    gradient = depth_back(fields, (split_pair(plain), split_pair(derived)))
    velocity_before = fetch.get("velocity")
    for n, value in enumerate(gradient):
        out[n] = velocity_before[n] - value


def swap(modes, axis):
    return lax.all_to_all(modes, axis, split_axis=0, concat_axis=0, tiled=True)


def after(value, *others):
    return lax.optimization_barrier((value, *others))


near, far = pl.BlockSpec(memory_space=pltpu.VMEM), pl.BlockSpec(memory_space=pltpu.HBM)


def in_hbm(value):
    return pltpu.with_memory_space_constraint(value, pltpu.HBM)


def fetching(body, out_shape, operands, specs, rows, extra=()):
    scratch = [pltpu.VMEM((count, 128), kind) for count, kind in rows]
    scratch += list(extra) + [pltpu.SemaphoreType.DMA((len(rows) + len(extra),))]
    return pl.pallas_call(
        body,
        out_shape=out_shape,
        in_specs=specs,
        scratch_shapes=scratch,
        compiler_params=pltpu.CompilerParams(vmem_limit_bytes=16 << 20),
    )(*[in_hbm(value) if spec is far else value for value, spec in zip(operands, specs)])


def table_rows(source, *names):
    found = []
    for name in names:
        high = max(b for (n, _), (_, b) in table_places.items() if n == name)
        found.append(source[table_places[name, 0][0] : high])
    return jnp.asarray(np.concatenate(found, 0))


def to_depth_modes(columns):
    shape = jax.ShapeDtypeStruct((32, 12, 128), bf16)
    return call(depth_kernel, shape, (columns, table_rows(narrow_tables, "depth", "depth_slope")))


def to_x_modes(modes):
    shape = jax.ShapeDtypeStruct((16, 16, 128), f32)
    tables = (table_rows(narrow_tables, "x"), table_rows(wide_tables, "turn_x"))
    return call(forward_kernel, shape, (modes, *tables))


def solve_y(modes, narrow, wide):
    shape = jax.ShapeDtypeStruct((16, 16, 128), f32)
    rows = [(512, bf16), (512, bf16), (48, f32), (8, f32), (8, f32)]
    return fetching(middle_kernel, shape, (modes, narrow, wide), [near, far, far], rows)


def from_x_modes(modes, narrow, wide):
    shape = jax.ShapeDtypeStruct((32, 12, 128), bf16)
    rows = [(512, bf16), (64, f32)]
    return fetching(backward_kernel, shape, (modes, narrow, wide), [near, far, far], rows)


def from_depth_modes(modes, columns):
    shape = jax.ShapeDtypeStruct((3, 128, 128), f32)
    table = table_rows(narrow_tables, "depth", "depth_back_slope")
    extra = [pltpu.VMEM((3, 128, 128), f32)]
    return fetching(last_kernel, shape, (modes, columns, table), [near, far, near], [], extra)


def pack_y_kernel(s_far, v_far, k_far, up, down, v, s, k, flags):
    fetch = Fetch()
    fetch.start("s", s_far, s, flags.at[0])
    fetch.start("v", v_far, v, flags.at[1])
    fetch.start("k", k_far, k, flags.at[2])
    for copy, _ in fetch.copies.values():
        copy.wait()
    for side, near, far in ((up, 15, 14), (down, 0, 1)):
        for n in range(20):
            side[n] = s[pl.ds(n * 128 + near, 8, stride=16), :].astype(bf16)
            side[20 + n] = s[pl.ds(n * 128 + far, 8, stride=16), :].astype(bf16)
        side[40] = k[pl.ds(near, 8, stride=16), :].astype(bf16)
        side[41] = k[pl.ds(far, 8, stride=16), :].astype(bf16)
        for n in range(3):
            side[42 + n] = v[pl.ds(n * 128 + near, 8, stride=16), :].astype(bf16)
            side[45 + n] = jnp.zeros((8, 128), bf16)


def pack_x_kernel(s, v, k, ylow, yhigh, up, down, edge, corner):
    edge[0] = ylow[...].astype(f32).reshape(384, 128)
    edge[1] = yhigh[...].astype(f32).reshape(384, 128)
    for side, near, far in ((up, 7, 6), (down, 0, 1)):
        for n in range(20):
            side[n] = s[n * 128 + near * 16 : n * 128 + near * 16 + 16].astype(bf16)
            side[20 + n] = s[n * 128 + far * 16 : n * 128 + far * 16 + 16].astype(bf16)
        side[40] = k[near * 16 : near * 16 + 16].astype(bf16)
        side[41] = k[far * 16 : far * 16 + 16].astype(bf16)
        for n in range(3):
            side[42 + n] = v[n * 128 + near * 16 : n * 128 + near * 16 + 16].astype(bf16)
        for m in range(2):
            for n in range(20):
                corner[20 * m + n : 20 * m + n + 1] = edge[m, n * 8 + near : n * 8 + near + 1]
            corner[40 + m : 41 + m] = edge[m, 320 + near : 321 + near]
        corner[42:48] = jnp.zeros((6, 128), f32)
        for n in range(3):
            side[45 + n] = corner[16 * n : 16 * n + 16].astype(bf16)


def shifted(value, row, step):
    count = value.shape[0]
    index = lax.broadcasted_iota(jnp.int32, value.shape, 0)
    if step > 0:
        return jnp.where(index == count - 1, row, pltpu.roll(value, count - 1, 0))
    return jnp.where(index == 0, row, pltpu.roll(value, 1, 0))


def weights_of(k, kxn, kxp, kyn, kyp, u, v, w):
    lane = lane_index(k.shape)
    last, first = lane == 127, lane == 0
    kzn = jnp.where(last, k, pltpu.roll(k, 127, 1))
    kzp = jnp.where(first, k, pltpu.roll(k, 1, 1))
    eighth = 0.5 * time_step
    half = 0.5 * eighth * 2.0
    xn, xp = half * (k + kxn - u), half * (k + kxp + u)
    yn, yp = half * (k + kyn - v), half * (k + kyp + v)
    zn, zp = half * (k + kzn - w), half * (k + kzp + w)
    own = 1.0 - half * (6.0 * k + kxn + kxp + kyn + kyp + kzn + kzp)
    own = own + jnp.where(last, zn, 0.0) + jnp.where(first, zp, 0.0)
    return own, xn, xp, yn, yp, jnp.where(last, 0.0, zn), jnp.where(first, 0.0, zp)


def stepped(c, f, xn, xp, yn, yp):
    total = c[0] * f + c[1] * xn + c[2] * xp
    total = total + (c[3] * yn + c[4] * yp)
    return total + (c[5] * pltpu.roll(f, 127, 1) + c[6] * pltpu.roll(f, 1, 1))


def transport_kernel(s_far, v, k, ylow, yhigh, xlow, xhigh, out, s, yf, xf, cx, cy, flags):
    fetch = Fetch()
    fetch.start("s", s_far, s, flags.at[0])
    yf[0] = ylow[...].astype(f32).reshape(384, 128)
    yf[1] = yhigh[...].astype(f32).reshape(384, 128)
    xf[0] = xlow[...].astype(f32).reshape(768, 128)
    xf[1] = xhigh[...].astype(f32).reshape(768, 128)

    def plane(side, n):
        return xf[side, 16 * n : 16 * n + 16]

    def strip(side, n):
        return yf[side, 8 * n : 8 * n + 8]

    ks = [plane(0, 41), plane(0, 40)] + [k[16 * n : 16 * n + 16] for n in range(8)] + [plane(1, 40), plane(1, 41)]
    for p in range(10):
        if p == 0 or p == 9:
            side = 0 if p == 0 else 1
            flow = [plane(side, 42 + n) for n in range(3)]
            row_low, row_high = xf[side, 760:761], xf[side, 761:762]
        else:
            x = p - 1
            flow = [v[n * 128 + 16 * x : n * 128 + 16 * x + 16] for n in range(3)]
            row_low, row_high = yf[0, 320 + x : 321 + x], yf[1, 320 + x : 321 + x]
        own = ks[p + 1]
        made = weights_of(
            own, ks[p + 2], ks[p], shifted(own, row_high, 1), shifted(own, row_low, -1), *flow
        )
        for n in range(7):
            cx[p, n] = made[n]
    for side in range(2):
        own = strip(side, 40)
        inner = k[pl.ds(15 * side, 8, stride=16), :]
        around = (inner, strip(0, 41)) if side == 0 else (strip(1, 41), inner)
        made = weights_of(
            own,
            shifted(own, xf[1, 760 + side : 761 + side], 1),
            shifted(own, xf[0, 760 + side : 761 + side], -1),
            *around,
            *[strip(side, 42 + n) for n in range(3)],
        )
        for n in range(7):
            cy[side, n] = made[n]

    def channel(n, carry):
        base = pl.multiple_of(n * 128, 128)

        def far_plane(side, m):
            return xf[side, pl.ds(pl.multiple_of(m * 16, 16), 16), :]

        def far_strip(side, m):
            return yf[side, pl.ds(pl.multiple_of(m * 8, 8), 8), :]

        fields = [s[pl.ds(base + 16 * x, 16), :] for x in range(8)]
        planes = [far_plane(0, 20 + n), far_plane(0, n)] + fields + [far_plane(1, n), far_plane(1, 20 + n)]
        strips = [far_strip(side, n) for side in range(2)]
        far = [far_strip(side, 20 + n) for side in range(2)]
        corners = [[xf[side, pl.ds(720 + 20 * m + n, 1), :] for m in range(2)] for side in range(2)]
        section = []
        for p in range(10):
            if p == 0 or p == 9:
                row_low, row_high = corners[0 if p == 0 else 1]
            else:
                row_low, row_high = strips[0][p - 1 : p], strips[1][p - 1 : p]
            own = planes[p + 1]
            section.append(
                stepped(
                    [cx[p, m] for m in range(7)],
                    own,
                    planes[p + 2],
                    planes[p],
                    shifted(own, row_high, 1),
                    shifted(own, row_low, -1),
                )
            )
        edges = []
        for side in range(2):
            own = strips[side]
            inner = s[pl.ds(base + 15 * side, 8, stride=16), :]
            around = (inner, far[0]) if side == 0 else (far[1], inner)
            edges.append(
                stepped(
                    [cy[side, m] for m in range(7)],
                    own,
                    shifted(own, corners[1][side], 1),
                    shifted(own, corners[0][side], -1),
                    *around,
                )
            )
        for x in range(8):
            own = section[x + 1]
            moved = stepped(
                [cx[x + 1, m] for m in range(7)],
                own,
                section[x + 2],
                section[x],
                shifted(own, edges[1][x : x + 1], 1),
                shifted(own, edges[0][x : x + 1], -1),
            )
            out[pl.ds(base + 16 * x, 16), :] = 0.5 * (fields[x] + moved)
        return carry

    fetch.copies["s"][0].wait()
    lax.fori_loop(0, 20, channel, 0)


def gelu_doubled(x):
    return x + x * jnp.tanh(x * (0.7978845608028654 + 0.035677408136300125 * (x * x)))


bundle = 16


def react_kernel(begin, end, listed, s, in_far, mid_far, out_far, out, w_in, w_mid, w_out, *rest):
    raw_in, raw_mid, raw_out, flags = rest
    fetch = Fetch()
    fetch.start("in", in_far, raw_in, flags.at[0])
    fetch.start("mid", mid_far, raw_mid, flags.at[1])
    fetch.start("out", out_far, raw_out, flags.at[2])
    out[...] = s[...]
    w_in[...] = fetch.get("in").astype(f32).T.astype(bf16)
    half = jnp.asarray(0.5, bf16)
    w_mid[...] = fetch.get("mid") * half
    w_out[...] = fetch.get("out") * half

    def step(g, carry):
        first = g * bundle

        @pl.when(listed[first] < 128)
        def _():
            places = [listed[first + q] for q in range(bundle)]
            bounded = [jnp.minimum(place, 127) for place in places]
            rows = [s[pl.ds(place, 20, stride=128), :] for place in bounded]
            feed = jnp.concatenate(rows, 1).astype(bf16)
            one = gelu_doubled(product(w_in[...], feed, ((1,), (0,)))).astype(bf16)
            two = gelu_doubled(product(w_mid[...], one, ((1,), (0,)))).astype(bf16)
            change = product(w_out[...], two, ((1,), (0,)))
            for q in range(bundle):

                @pl.when(places[q] < 128)
                def _():
                    out[pl.ds(bounded[q], 20, stride=128), :] = (
                        rows[q] + change[:, 128 * q : 128 * q + 128]
                    )

        return carry

    lax.fori_loop(begin // bundle, end // bundle, step, 0)


def exchange(up, down, axis):
    size = lax.axis_size(axis)
    forward = [(n, (n + 1) % size) for n in range(size)]
    low = lax.ppermute(up, axis, forward)
    return low, lax.ppermute(down, axis, [(b, a) for a, b in forward])


def pack_y(s, v, k):
    strip = jax.ShapeDtypeStruct((48, 8, 128), bf16)
    return pl.pallas_call(
        pack_y_kernel,
        out_shape=(strip, strip, jax.ShapeDtypeStruct((384, 128), f32)),
        in_specs=[far] * 3,
        out_specs=(near,) * 3,
        scratch_shapes=[
            pltpu.VMEM((2560, 128), f32),
            pltpu.VMEM((128, 128), f32),
            pltpu.SemaphoreType.DMA((3,)),
        ],
        compiler_params=pltpu.CompilerParams(vmem_limit_bytes=16 << 20),
        name="pack_y",
    )(in_hbm(s), in_hbm(v), in_hbm(k))


def pack_x(s, v, k, ylow, yhigh):
    face = jax.ShapeDtypeStruct((48, 16, 128), bf16)
    return pl.pallas_call(
        pack_x_kernel,
        out_shape=(face, face),
        scratch_shapes=[pltpu.VMEM((2, 384, 128), f32), pltpu.VMEM((48, 128), f32)],
        compiler_params=pltpu.CompilerParams(vmem_limit_bytes=16 << 20),
        name="pack_x",
    )(s, v, k, ylow, yhigh)


def transport(s, v, k, strips, faces):
    return pl.pallas_call(
        transport_kernel,
        out_shape=jax.ShapeDtypeStruct((2560, 128), f32),
        in_specs=[far] + [near] * 6,
        scratch_shapes=[
            pltpu.VMEM((2560, 128), f32),
            pltpu.VMEM((2, 384, 128), f32),
            pltpu.VMEM((2, 768, 128), f32),
            pltpu.VMEM((10, 7, 16, 128), f32),
            pltpu.VMEM((2, 7, 8, 128), f32),
            pltpu.SemaphoreType.DMA((1,)),
        ],
        compiler_params=pltpu.CompilerParams(vmem_limit_bytes=24 << 20),
        name="transport",
    )(in_hbm(s), v, k, *strips, *faces)


def react(moved, listed, network, begin, end):
    w_in, w_mid, w_out = network
    return pl.pallas_call(
        functools.partial(react_kernel, begin, end),
        out_shape=jax.ShapeDtypeStruct((2560, 128), f32),
        in_specs=[pl.BlockSpec(memory_space=pltpu.SMEM), near, far, far, far],
        scratch_shapes=[
            pltpu.VMEM((800, 20), bf16),
            pltpu.VMEM((400, 800), bf16),
            pltpu.VMEM((20, 400), bf16),
            pltpu.VMEM((20, 800), bf16),
            pltpu.VMEM((400, 800), bf16),
            pltpu.VMEM((20, 400), bf16),
            pltpu.SemaphoreType.DMA((3,)),
        ],
        compiler_params=pltpu.CompilerParams(vmem_limit_bytes=48 << 20),
        name="react",
    )(listed, moved, in_hbm(w_in.T), in_hbm(w_mid), in_hbm(w_out))


def advance(scalars, velocity, diffusivity, burn_list, w_in, w_mid, w_out):
    s = scalars.reshape(2560, 128)
    v = velocity.reshape(384, 128)
    k = diffusivity.reshape(128, 128)
    listed = burn_list.reshape(64)
    up, down, kept = pack_y(s, v, k)
    narrow, wide = jnp.asarray(narrow_tables), jnp.asarray(wide_tables)
    network = (w_in, w_mid, w_out)
    strips = exchange(up, down, "gy")
    modes = to_depth_modes(kept.reshape(3, 128, 128))
    modes = swap(modes, "gx")
    up, down = pack_x(s, v, k, *strips)
    faces = exchange(up, down, "gx")
    modes, up, down = after(modes, up, down)
    modes = to_x_modes(modes)
    modes = swap(modes, "gy")
    moved = transport(s, v, k, strips, faces)
    modes, moved = after(modes, moved)
    modes = swap(solve_y(modes, narrow, wide), "gy")
    moved = react(moved, listed, network, 0, early_slots)
    modes, moved = after(modes, moved)
    modes = swap(from_x_modes(modes, narrow, wide), "gx")
    moved = react(moved, listed, network, early_slots, 64)
    velocity_out = from_depth_modes(modes, velocity.reshape(3, 128, 128))
    return (moved.reshape(scalars.shape), velocity_out.reshape(velocity.shape))


def solution(mesh):
    in_specs = (
        P(None, "gx", "gy", None),
        P(None, "gx", "gy", None),
        P("gx", "gy", None),
        P("gx", "gy", None),
        P(),
        P(),
        P(),
    )
    out_specs = (P(None, "gx", "gy", None), P(None, "gx", "gy", None))
    return jax.shard_map(advance, mesh=mesh, in_specs=in_specs, out_specs=out_specs, check_vma=False)
```

```python
import functools
import math

import jax
import jax.numpy as jnp
import numpy as np
from jax import lax
from jax.experimental import pallas as pl
from jax.experimental.pallas import tpu as pltpu
from jax.sharding import PartitionSpec as P


time_step = 0.25
early_slots = 16
f32 = jnp.float32
bf16 = jnp.bfloat16


def split_table(table):
    high = np.asarray(table, np.float64).astype(jnp.bfloat16)
    low = (np.asarray(table, np.float64) - high.astype(np.float64)).astype(jnp.bfloat16)
    return high, low


def product(left, right, contract):
    return lax.dot_general(left, right, (contract, ((), ())), preferred_element_type=f32)


def halves(value):
    high = value.astype(bf16)
    return high, (value - high.astype(f32)).astype(bf16)


def right_table(value, table_high, table_low):
    contract = ((1,), (0,))
    high, low = halves(value)
    return (
        product(high, table_high, contract)
        + product(low, table_high, contract)
        + product(high, table_low, contract)
    )


def times(pair, factor):
    real, imag = pair
    c, s = float(np.real(factor)), float(np.imag(factor))
    if abs(s) < 1e-12:
        return (real, imag) if c > 0 else (-real, -imag)
    if abs(c) < 1e-12:
        return (-imag, real) if s > 0 else (imag, -real)
    if abs(abs(c) - abs(s)) < 1e-12:
        size = abs(c)
        sc, ss = (1 if c > 0 else -1), (1 if s > 0 else -1)
        first = real * size
        second = imag * size
        new_real = (first if sc > 0 else -first) - (second if ss > 0 else -second)
        new_imag = (first if ss > 0 else -first) + (second if sc > 0 else -second)
        return new_real, new_imag
    return real * c - imag * s, real * s + imag * c


def complex_dft(values):
    count = len(values)
    if count == 1:
        return values
    even = complex_dft(values[0::2])
    odd = complex_dft(values[1::2])
    half = count // 2
    low, high = [], []
    for k in range(half):
        turned = times(odd[k], np.exp(-2j * np.pi * k / count))
        low.append((even[k][0] + turned[0], even[k][1] + turned[1]))
        high.append((even[k][0] - turned[0], even[k][1] - turned[1]))
    return low + high


def real_dft(values):
    count = len(values)
    if count == 2:
        zero = jnp.zeros_like(values[0])
        return [(values[0] + values[1], zero), (values[0] - values[1], zero)]
    even = real_dft(values[0::2])
    odd = real_dft(values[1::2])
    half = count // 2
    out = [None] * (half + 1)
    for k in range(half // 2 + 1):
        turned = times(odd[k], np.exp(-2j * np.pi * k / count))
        out[half - k] = (even[k][0] - turned[0], turned[1] - even[k][1])
        out[k] = (even[k][0] + turned[0], even[k][1] + turned[1])
    return out


def full_spectrum(values):
    half = real_dft(values)
    count = len(values)
    return [half[k] if k <= count // 2 else (half[count - k][0], -half[count - k][1]) for k in range(count)]


def turn(pair, cosine, sine):
    real, imag = pair
    return real * cosine + imag * sine, imag * cosine - real * sine


def lane_index(shape):
    return lax.broadcasted_iota(jnp.int32, shape, len(shape) - 1)


def central(values, step, roll):
    count = len(values)
    lane = lane_index(values[0].shape)
    if step == 16:
        digit, top = lane // 16, 7
        forward_from_other, backward_from_other = -16, 16
    else:
        digit, top = lane % 16, 15
        forward_from_other, backward_from_other = 15, -15
    last, first = digit == top, digit == 0
    up = [roll(v, -step) for v in values]
    down = [roll(v, step) for v in values]
    up_other = up if step == 16 else [roll(v, forward_from_other) for v in values]
    down_other = down if step == 16 else [roll(v, backward_from_other) for v in values]
    out = []
    for n in range(count):
        after = jnp.where(last, up_other[(n + 1) % count], up[n])
        before = jnp.where(first, down_other[(n - 1) % count], down[n])
        out.append(0.5 * (after - before))
    return out


def depth_modes(velocity, tables):
    plain, derived = tables
    fields = []
    for n in range(3):
        table_high, table_low = plain if n < 2 else derived
        high, low = halves(velocity[n])
        contract = ((1,), (1,))
        fields.append(
            product(table_high, high, contract)
            + product(table_high, low, contract)
            + product(table_low, high, contract)
        )
    return [
        jnp.concatenate([f[4 * n : 4 * n + 4] for f in fields], 0) for n in range(32)
    ]


def forward_x(values, turn_cos, turn_sin, roll):
    slope = central([v[0:8] for v in values], 16, roll)
    lines = [
        jnp.concatenate([s[0:4] + v[8:12], v[4:8]], 0) for s, v in zip(slope, values)
    ]
    modes = full_spectrum(lines)
    rows = []
    for k, pair in enumerate(modes):
        rows.append(jnp.concatenate(turn(pair, turn_cos[k : k + 1], turn_sin[k : k + 1]), 1))
    return jnp.concatenate(rows, 0)


def middle_y(values, fetch, roll):
    plain = [jnp.concatenate([v[0:4], v[8:12]], 0) for v in values]
    other = [jnp.concatenate([v[4:8], v[12:16]], 0) for v in values]
    lines = [p + s for p, s in zip(plain, central(other, 1, roll))]
    rows = []
    turns = fetch.get("turn")
    turn_cos, turn_sin, eigen_y = turns[:16], turns[16:32], turns[32:48]
    for k, pair in enumerate(full_spectrum(lines)):
        rows.append(jnp.concatenate(turn(pair, turn_cos[k : k + 1], turn_sin[k : k + 1]), 1))
    modes = right_table(jnp.concatenate(rows, 0), *split_pair(fetch.get("y")))
    eigen_xz = fetch.get("ex") + fetch.get("ez")
    scaled = []
    for k in range(16):
        eigen = eigen_xz + eigen_y[k : k + 1]
        mean_mode = eigen == 0.0
        scale = jnp.where(mean_mode, 0.0, (-1.0 / 65536.0) / jnp.where(mean_mode, 1.0, eigen))
        scaled.append(modes[8 * k : 8 * k + 8] * scale)
    back = right_table(jnp.concatenate(scaled, 0), *split_doubled(fetch.get("y_back")))
    pairs = []
    for k in range(16):
        row = back[8 * k : 8 * k + 8]
        pairs.append(turn((row[:, :128], row[:, 128:]), turn_cos[k : k + 1], turn_sin[k : k + 1]))
    pressure = [real - imag for real, imag in complex_dft(pairs)]
    slope = central(pressure, 1, roll)
    return [
        jnp.concatenate([p[0:4], s[0:4], p[4:8], s[4:8]], 0) for p, s in zip(pressure, slope)
    ]


def backward_x(modes, table_back, turn_cos, turn_sin, roll):
    back = right_table(modes, *table_back)
    pairs = []
    for k in range(32):
        row = back[8 * k : 8 * k + 8]
        pairs.append(turn((row[:, :128], row[:, 128:]), turn_cos[k : k + 1], turn_sin[k : k + 1]))
    lines = [real - imag for real, imag in complex_dft(pairs)]
    slope = central(lines, 16, roll)
    return [
        jnp.concatenate([s[0:4], v[4:8], v[0:4]], 0) for s, v in zip(slope, lines)
    ]


def depth_back(fields, tables):
    plain, derived = tables
    out = []
    for n in range(3):
        table_high, table_low = plain if n < 2 else derived
        turned = fields[n].T.astype(bf16)
        contract = ((1,), (0,))
        out.append(product(turned, table_high, contract) + product(turned, table_low, contract))
    return out


def cosine_numpy(length):
    position = np.arange(length)
    weight = np.where(position == 0, math.sqrt(1.0 / length), math.sqrt(2.0 / length))
    return weight[:, None] * np.cos(np.pi / (2 * length) * position[:, None] * (2 * position[None, :] + 1))


def make_tables():
    t = {}
    cosine = cosine_numpy(128)
    above = np.concatenate([cosine[:, 1:], cosine[:, -1:]], 1)
    below = np.concatenate([cosine[:, :1], cosine[:, :-1]], 1)
    t["depth"] = split_table(cosine)
    t["depth_back_slope"] = split_table(0.5 * (above - below))
    slope = np.zeros((128, 128))
    for z in range(128):
        slope[z, min(z + 1, 127)] += 0.5
        slope[z, max(z - 1, 0)] -= 0.5
    t["depth_slope"] = split_table(cosine @ slope)

    def digits(points):
        angle = 2 * np.pi / points * np.outer(np.arange(points), np.arange(points))
        return angle

    eight, sixteen = digits(8), digits(16)
    one16, one8 = np.eye(16), np.eye(8)
    t["x"] = split_table(
        np.concatenate(
            [np.kron(np.cos(eight) + np.sin(eight), one16), np.kron(np.sin(eight) - np.cos(eight), one16)], 0
        )
    )
    t["y"] = split_table(
        np.concatenate(
            [np.kron(one8, np.cos(sixteen) + np.sin(sixteen)), np.kron(one8, np.sin(sixteen) - np.cos(sixteen))], 0
        )
    )
    t["x_back"] = split_table(
        np.concatenate([np.kron(np.cos(eight), one16), np.kron(-np.sin(eight), one16)], 1)
    )
    t["y_back"] = split_table(
        np.concatenate([np.kron(one8, np.cos(sixteen)), np.kron(one8, -np.sin(sixteen))], 1)
    )
    lane = np.arange(128)
    turn_x = 2 * np.pi / 256 * np.outer(np.arange(32), lane // 16)
    turn_y = 2 * np.pi / 256 * np.outer(np.arange(16), lane % 16)
    t["turn_x"] = (np.cos(turn_x).astype(np.float32), np.sin(turn_x).astype(np.float32))
    t["turn_y"] = (np.cos(turn_y).astype(np.float32), np.sin(turn_y).astype(np.float32))
    k1 = np.arange(32)
    eigen_x = 2 - 2 * np.cos(2 * np.pi / 256 * (k1[:, None] + 32 * (lane // 16)[None, :]))
    t["eigen_x"] = np.repeat(eigen_x.reshape(16, 2, 128), 4, axis=1).astype(np.float32)
    kz = 2 - 2 * np.cos(np.pi * np.arange(128) / 128)
    t["eigen_z"] = np.ascontiguousarray(
        np.broadcast_to(np.tile(kz.reshape(32, 4), (1, 2))[:, :, None], (32, 8, 128))
    ).astype(np.float32)
    t["eigen_y"] = (
        2 - 2 * np.cos(2 * np.pi / 256 * (np.arange(16)[:, None] + 16 * (lane % 16)[None, :]))
    ).astype(np.float32)
    return t


def lane_roll(value, shift):
    return pltpu.roll(value, shift % 128, 1)


def call(body, out_shape, operands, limit=16):
    return pl.pallas_call(
        body,
        out_shape=out_shape,
        compiler_params=pltpu.CompilerParams(vmem_limit_bytes=limit << 20),
    )(*operands)


def pack_tables():
    t = make_tables()
    places, narrow, wide = {}, [], []
    at = 0
    for name in ("depth", "depth_slope", "depth_back_slope", "x", "y", "x_back", "y_back"):
        for n, table in enumerate(t[name]):
            if table.shape[1] == 256:
                table = np.concatenate([table[:, :128], table[:, 128:]], 0)
            places[name, n] = (at, at + table.shape[0])
            narrow.append(table)
            at += table.shape[0]
    at = 0
    for name in ("turn_x", "turn_y", "eigen_y", "eigen_x", "eigen_z"):
        parts = t[name] if isinstance(t[name], tuple) else (t[name],)
        for n, table in enumerate(parts):
            table = table.reshape(-1, 128)
            places[name, n] = (at, at + table.shape[0])
            wide.append(table)
            at += table.shape[0]
    return places, np.concatenate(narrow, 0), np.concatenate(wide, 0)


table_places, narrow_tables, wide_tables = pack_tables()


class Fetch:
    def __init__(self):
        self.copies = {}

    def start(self, name, source, target, flag):
        copy = pltpu.make_async_copy(source, target, flag)
        copy.start()
        self.copies[name] = (copy, target)

    def get(self, name):
        copy, target = self.copies[name]
        copy.wait()
        return target[...]


def split_pair(table):
    half = table.shape[0] // 2
    return table[:half], table[half:]


def split_doubled(table):
    return tuple(jnp.concatenate([half[:128], half[128:]], 1) for half in split_pair(table))


def depth_kernel(velocity, table, out):
    plain, derived = split_pair(table[...])
    groups = depth_modes([velocity[n] for n in range(3)], (split_pair(plain), split_pair(derived)))
    for n, group in enumerate(groups):
        out[n] = group.astype(bf16)


def forward_kernel(values, table, turns, out):
    loaded = [values[n].astype(f32) for n in range(32)]
    rows = forward_x(loaded, *split_pair(turns[...]), lane_roll)
    modes = right_table(rows, *split_pair(table[...]))
    out[...] = modes.reshape(16, 16, 128)


class Held:
    def __init__(self, fetch, **held):
        self.fetch, self.held = fetch, held

    def get(self, name):
        return self.held[name][...] if name in self.held else self.fetch.get(name)


def middle_kernel(values, table, back, turns, wide, out, ex, ez, flags):
    fetch = Fetch()
    at_x = pl.multiple_of(table_places["eigen_x", 0][0] + 8 * lax.axis_index("gy"), 8)
    at_z = pl.multiple_of(table_places["eigen_z", 0][0] + 8 * lax.axis_index("gx"), 8)
    fetch.start("ex", wide.at[pl.ds(at_x, 8)], ex, flags.at[0])
    fetch.start("ez", wide.at[pl.ds(at_z, 8)], ez, flags.at[1])
    tables = Held(fetch, y=table, y_back=back, turn=turns)
    result = middle_y([values[n] for n in range(16)], tables, lane_roll)
    for n, value in enumerate(result):
        out[n] = value


def backward_kernel(values, table, turns, out):
    result = backward_x(
        values[...].reshape(256, 128), split_doubled(table[...]), *split_pair(turns[...]), lane_roll
    )
    for n, value in enumerate(result):
        out[n] = value.astype(bf16)


def last_kernel(values, velocity, table, out):
    loaded = [values[n].astype(f32) for n in range(32)]
    fields = [jnp.concatenate([v[4 * n : 4 * n + 4] for v in loaded], 0) for n in range(3)]
    plain, derived = split_pair(table[...])
    gradient = depth_back(fields, (split_pair(plain), split_pair(derived)))
    for n, value in enumerate(gradient):
        out[n] = velocity[n] - value


def swap(modes, axis):
    return lax.all_to_all(modes, axis, split_axis=0, concat_axis=0, tiled=True)


def after(value, *others):
    return lax.optimization_barrier((value, *others))


near, far = pl.BlockSpec(memory_space=pltpu.VMEM), pl.BlockSpec(memory_space=pltpu.HBM)


def in_hbm(value):
    return pltpu.with_memory_space_constraint(value, pltpu.HBM)


def fetching(body, out_shape, operands, specs, rows, extra=()):
    scratch = [pltpu.VMEM((count, 128), kind) for count, kind in rows]
    scratch += list(extra) + [pltpu.SemaphoreType.DMA((len(rows) + len(extra),))]
    return pl.pallas_call(
        body,
        out_shape=out_shape,
        in_specs=specs,
        scratch_shapes=scratch,
        compiler_params=pltpu.CompilerParams(vmem_limit_bytes=16 << 20),
    )(*[in_hbm(value) if spec is far else value for value, spec in zip(operands, specs)])


def table_rows(source, *names):
    found = []
    for name in names:
        high = max(b for (n, _), (_, b) in table_places.items() if n == name)
        found.append(source[table_places[name, 0][0] : high])
    return jnp.asarray(np.concatenate(found, 0))


def to_depth_modes(columns):
    shape = jax.ShapeDtypeStruct((32, 12, 128), bf16)
    return call(depth_kernel, shape, (columns, table_rows(narrow_tables, "depth", "depth_slope")))


def to_x_modes(modes):
    shape = jax.ShapeDtypeStruct((16, 16, 128), f32)
    tables = (table_rows(narrow_tables, "x"), table_rows(wide_tables, "turn_x"))
    return call(forward_kernel, shape, (modes, *tables))


def solve_y(modes, wide):
    shape = jax.ShapeDtypeStruct((16, 16, 128), f32)
    tables = [table_rows(narrow_tables, name) for name in ("y", "y_back")]
    tables.append(table_rows(wide_tables, "turn_y", "eigen_y"))
    rows = [(8, f32), (8, f32)]
    return fetching(middle_kernel, shape, (modes, *tables, wide), [near] * 4 + [far], rows)


def from_x_modes(modes):
    shape = jax.ShapeDtypeStruct((32, 12, 128), bf16)
    tables = (table_rows(narrow_tables, "x_back"), table_rows(wide_tables, "turn_x"))
    return call(backward_kernel, shape, (modes, *tables))


def from_depth_modes(modes, columns):
    shape = jax.ShapeDtypeStruct((3, 128, 128), f32)
    table = table_rows(narrow_tables, "depth", "depth_back_slope")
    return call(last_kernel, shape, (modes, columns, table))


def pack_y_kernel(s_far, v_far, k_far, up, down, v, s, k, flags):
    fetch = Fetch()
    fetch.start("s", s_far, s, flags.at[0])
    fetch.start("v", v_far, v, flags.at[1])
    fetch.start("k", k_far, k, flags.at[2])
    for copy, _ in fetch.copies.values():
        copy.wait()
    for side, near, far in ((up, 15, 14), (down, 0, 1)):
        for n in range(20):
            side[n] = s[pl.ds(n * 128 + near, 8, stride=16), :].astype(bf16)
            side[20 + n] = s[pl.ds(n * 128 + far, 8, stride=16), :].astype(bf16)
        side[40] = k[pl.ds(near, 8, stride=16), :].astype(bf16)
        side[41] = k[pl.ds(far, 8, stride=16), :].astype(bf16)
        for n in range(3):
            side[42 + n] = v[pl.ds(n * 128 + near, 8, stride=16), :].astype(bf16)
            side[45 + n] = jnp.zeros((8, 128), bf16)


def pack_x_kernel(s, v, k, ylow, yhigh, up, down, edge, corner):
    edge[0] = ylow[...].astype(f32).reshape(384, 128)
    edge[1] = yhigh[...].astype(f32).reshape(384, 128)
    for side, near, far in ((up, 7, 6), (down, 0, 1)):
        for n in range(20):
            side[n] = s[n * 128 + near * 16 : n * 128 + near * 16 + 16].astype(bf16)
            side[20 + n] = s[n * 128 + far * 16 : n * 128 + far * 16 + 16].astype(bf16)
        side[40] = k[near * 16 : near * 16 + 16].astype(bf16)
        side[41] = k[far * 16 : far * 16 + 16].astype(bf16)
        for n in range(3):
            side[42 + n] = v[n * 128 + near * 16 : n * 128 + near * 16 + 16].astype(bf16)
        for m in range(2):
            for n in range(20):
                corner[20 * m + n : 20 * m + n + 1] = edge[m, n * 8 + near : n * 8 + near + 1]
            corner[40 + m : 41 + m] = edge[m, 320 + near : 321 + near]
        corner[42:48] = jnp.zeros((6, 128), f32)
        for n in range(3):
            side[45 + n] = corner[16 * n : 16 * n + 16].astype(bf16)


def shifted(value, row, step):
    count = value.shape[0]
    index = lax.broadcasted_iota(jnp.int32, value.shape, 0)
    if step > 0:
        return jnp.where(index == count - 1, row, pltpu.roll(value, count - 1, 0))
    return jnp.where(index == 0, row, pltpu.roll(value, 1, 0))


def weights_of(k, kxn, kxp, kyn, kyp, u, v, w):
    lane = lane_index(k.shape)
    last, first = lane == 127, lane == 0
    kzn = jnp.where(last, k, pltpu.roll(k, 127, 1))
    kzp = jnp.where(first, k, pltpu.roll(k, 1, 1))
    eighth = 0.5 * time_step
    half = 0.5 * eighth * 2.0
    xn, xp = half * (k + kxn - u), half * (k + kxp + u)
    yn, yp = half * (k + kyn - v), half * (k + kyp + v)
    zn, zp = half * (k + kzn - w), half * (k + kzp + w)
    own = 1.0 - half * (6.0 * k + kxn + kxp + kyn + kyp + kzn + kzp)
    own = own + jnp.where(last, zn, 0.0) + jnp.where(first, zp, 0.0)
    return own, xn, xp, yn, yp, jnp.where(last, 0.0, zn), jnp.where(first, 0.0, zp)


def stepped(c, f, xn, xp, yn, yp):
    total = c[0] * f + c[1] * xn + c[2] * xp
    total = total + (c[3] * yn + c[4] * yp)
    return total + (c[5] * pltpu.roll(f, 127, 1) + c[6] * pltpu.roll(f, 1, 1))


def transport_kernel(s_far, v, k, ylow, yhigh, xlow, xhigh, out, s, yf, xf, cx, cy, flags):
    fetch = Fetch()
    fetch.start("s", s_far, s, flags.at[0])
    yf[0] = ylow[...].astype(f32).reshape(384, 128)
    yf[1] = yhigh[...].astype(f32).reshape(384, 128)
    xf[0] = xlow[...].astype(f32).reshape(768, 128)
    xf[1] = xhigh[...].astype(f32).reshape(768, 128)

    def plane(side, n):
        return xf[side, 16 * n : 16 * n + 16]

    def strip(side, n):
        return yf[side, 8 * n : 8 * n + 8]

    ks = [plane(0, 41), plane(0, 40)] + [k[16 * n : 16 * n + 16] for n in range(8)] + [plane(1, 40), plane(1, 41)]
    for p in range(10):
        if p == 0 or p == 9:
            side = 0 if p == 0 else 1
            flow = [plane(side, 42 + n) for n in range(3)]
            row_low, row_high = xf[side, 760:761], xf[side, 761:762]
        else:
            x = p - 1
            flow = [v[n * 128 + 16 * x : n * 128 + 16 * x + 16] for n in range(3)]
            row_low, row_high = yf[0, 320 + x : 321 + x], yf[1, 320 + x : 321 + x]
        own = ks[p + 1]
        made = weights_of(
            own, ks[p + 2], ks[p], shifted(own, row_high, 1), shifted(own, row_low, -1), *flow
        )
        for n in range(7):
            cx[p, n] = made[n]
    for side in range(2):
        own = strip(side, 40)
        inner = k[pl.ds(15 * side, 8, stride=16), :]
        around = (inner, strip(0, 41)) if side == 0 else (strip(1, 41), inner)
        made = weights_of(
            own,
            shifted(own, xf[1, 760 + side : 761 + side], 1),
            shifted(own, xf[0, 760 + side : 761 + side], -1),
            *around,
            *[strip(side, 42 + n) for n in range(3)],
        )
        for n in range(7):
            cy[side, n] = made[n]

    def channel(n, carry):
        base = pl.multiple_of(n * 128, 128)

        def far_plane(side, m):
            return xf[side, pl.ds(pl.multiple_of(m * 16, 16), 16), :]

        def far_strip(side, m):
            return yf[side, pl.ds(pl.multiple_of(m * 8, 8), 8), :]

        fields = [s[pl.ds(base + 16 * x, 16), :] for x in range(8)]
        planes = [far_plane(0, 20 + n), far_plane(0, n)] + fields + [far_plane(1, n), far_plane(1, 20 + n)]
        strips = [far_strip(side, n) for side in range(2)]
        far = [far_strip(side, 20 + n) for side in range(2)]
        corners = [[xf[side, pl.ds(720 + 20 * m + n, 1), :] for m in range(2)] for side in range(2)]
        section = []
        for p in range(10):
            if p == 0 or p == 9:
                row_low, row_high = corners[0 if p == 0 else 1]
            else:
                row_low, row_high = strips[0][p - 1 : p], strips[1][p - 1 : p]
            own = planes[p + 1]
            section.append(
                stepped(
                    [cx[p, m] for m in range(7)],
                    own,
                    planes[p + 2],
                    planes[p],
                    shifted(own, row_high, 1),
                    shifted(own, row_low, -1),
                )
            )
        edges = []
        for side in range(2):
            own = strips[side]
            inner = s[pl.ds(base + 15 * side, 8, stride=16), :]
            around = (inner, far[0]) if side == 0 else (far[1], inner)
            edges.append(
                stepped(
                    [cy[side, m] for m in range(7)],
                    own,
                    shifted(own, corners[1][side], 1),
                    shifted(own, corners[0][side], -1),
                    *around,
                )
            )
        for x in range(8):
            own = section[x + 1]
            moved = stepped(
                [cx[x + 1, m] for m in range(7)],
                own,
                section[x + 2],
                section[x],
                shifted(own, edges[1][x : x + 1], 1),
                shifted(own, edges[0][x : x + 1], -1),
            )
            out[pl.ds(base + 16 * x, 16), :] = 0.5 * (fields[x] + moved)
        return carry

    fetch.copies["s"][0].wait()
    lax.fori_loop(0, 20, channel, 0)


def gelu_doubled(x):
    return x + x * jnp.tanh(x * (0.7978845608028654 + 0.035677408136300125 * (x * x)))


bundle = 16


def react_kernel(begin, end, listed, s, in_far, mid_far, out_far, out, w_in, w_mid, w_out, *rest):
    raw_in, raw_mid, raw_out, flags = rest
    fetch = Fetch()
    fetch.start("in", in_far, raw_in, flags.at[0])
    fetch.start("mid", mid_far, raw_mid, flags.at[1])
    fetch.start("out", out_far, raw_out, flags.at[2])
    out[...] = s[...]
    w_in[...] = fetch.get("in").astype(f32).T.astype(bf16)
    half = jnp.asarray(0.5, bf16)
    w_mid[...] = fetch.get("mid") * half
    w_out[...] = fetch.get("out") * half

    def step(g, carry):
        first = g * bundle

        @pl.when(listed[first] < 128)
        def _():
            places = [listed[first + q] for q in range(bundle)]
            bounded = [jnp.minimum(place, 127) for place in places]
            rows = [s[pl.ds(place, 20, stride=128), :] for place in bounded]
            feed = jnp.concatenate(rows, 1).astype(bf16)
            one = gelu_doubled(product(w_in[...], feed, ((1,), (0,)))).astype(bf16)
            two = gelu_doubled(product(w_mid[...], one, ((1,), (0,)))).astype(bf16)
            change = product(w_out[...], two, ((1,), (0,)))
            for q in range(bundle):

                @pl.when(places[q] < 128)
                def _():
                    out[pl.ds(bounded[q], 20, stride=128), :] = (
                        rows[q] + change[:, 128 * q : 128 * q + 128]
                    )

        return carry

    lax.fori_loop(begin // bundle, end // bundle, step, 0)


def exchange(up, down, axis):
    size = lax.axis_size(axis)
    forward = [(n, (n + 1) % size) for n in range(size)]
    low = lax.ppermute(up, axis, forward)
    return low, lax.ppermute(down, axis, [(b, a) for a, b in forward])


def pack_y(s, v, k):
    strip = jax.ShapeDtypeStruct((48, 8, 128), bf16)
    return pl.pallas_call(
        pack_y_kernel,
        out_shape=(strip, strip, jax.ShapeDtypeStruct((384, 128), f32)),
        in_specs=[far] * 3,
        out_specs=(near,) * 3,
        scratch_shapes=[
            pltpu.VMEM((2560, 128), f32),
            pltpu.VMEM((128, 128), f32),
            pltpu.SemaphoreType.DMA((3,)),
        ],
        compiler_params=pltpu.CompilerParams(vmem_limit_bytes=16 << 20),
        name="pack_y",
    )(in_hbm(s), in_hbm(v), in_hbm(k))


def pack_x(s, v, k, ylow, yhigh):
    face = jax.ShapeDtypeStruct((48, 16, 128), bf16)
    return pl.pallas_call(
        pack_x_kernel,
        out_shape=(face, face),
        scratch_shapes=[pltpu.VMEM((2, 384, 128), f32), pltpu.VMEM((48, 128), f32)],
        compiler_params=pltpu.CompilerParams(vmem_limit_bytes=16 << 20),
        name="pack_x",
    )(s, v, k, ylow, yhigh)


def transport(s, v, k, strips, faces):
    return pl.pallas_call(
        transport_kernel,
        out_shape=jax.ShapeDtypeStruct((2560, 128), f32),
        in_specs=[far] + [near] * 6,
        scratch_shapes=[
            pltpu.VMEM((2560, 128), f32),
            pltpu.VMEM((2, 384, 128), f32),
            pltpu.VMEM((2, 768, 128), f32),
            pltpu.VMEM((10, 7, 16, 128), f32),
            pltpu.VMEM((2, 7, 8, 128), f32),
            pltpu.SemaphoreType.DMA((1,)),
        ],
        compiler_params=pltpu.CompilerParams(vmem_limit_bytes=24 << 20),
        name="transport",
    )(in_hbm(s), v, k, *strips, *faces)


def react(moved, listed, network, begin, end):
    w_in, w_mid, w_out = network
    return pl.pallas_call(
        functools.partial(react_kernel, begin, end),
        out_shape=jax.ShapeDtypeStruct((2560, 128), f32),
        in_specs=[pl.BlockSpec(memory_space=pltpu.SMEM), near, far, far, far],
        scratch_shapes=[
            pltpu.VMEM((800, 20), bf16),
            pltpu.VMEM((400, 800), bf16),
            pltpu.VMEM((20, 400), bf16),
            pltpu.VMEM((20, 800), bf16),
            pltpu.VMEM((400, 800), bf16),
            pltpu.VMEM((20, 400), bf16),
            pltpu.SemaphoreType.DMA((3,)),
        ],
        compiler_params=pltpu.CompilerParams(vmem_limit_bytes=48 << 20),
        name="react",
    )(listed, moved, in_hbm(w_in.T), in_hbm(w_mid), in_hbm(w_out))


def advance(scalars, velocity, diffusivity, burn_list, w_in, w_mid, w_out):
    s = scalars.reshape(2560, 128)
    v = velocity.reshape(384, 128)
    k = diffusivity.reshape(128, 128)
    listed = burn_list.reshape(64)
    up, down, kept = pack_y(s, v, k)
    wide = jnp.asarray(wide_tables)
    network = (w_in, w_mid, w_out)
    strips = exchange(up, down, "gy")
    modes = to_depth_modes(kept.reshape(3, 128, 128))
    modes = swap(modes, "gx")
    up, down = pack_x(s, v, k, *strips)
    faces = exchange(up, down, "gx")
    modes, up, down = after(modes, up, down)
    modes = to_x_modes(modes)
    modes = swap(modes, "gy")
    moved = transport(s, v, k, strips, faces)
    modes, moved = after(modes, moved)
    modes = swap(solve_y(modes, wide), "gy")
    moved = react(moved, listed, network, 0, early_slots)
    modes, moved = after(modes, moved)
    modes = swap(from_x_modes(modes), "gx")
    moved = react(moved, listed, network, early_slots, 64)
    velocity_out = from_depth_modes(modes, velocity.reshape(3, 128, 128))
    return (moved.reshape(scalars.shape), velocity_out.reshape(velocity.shape))


def solution(mesh):
    in_specs = (
        P(None, "gx", "gy", None),
        P(None, "gx", "gy", None),
        P("gx", "gy", None),
        P("gx", "gy", None),
        P(),
        P(),
        P(),
    )
    out_specs = (P(None, "gx", "gy", None), P(None, "gx", "gy", None))
    return jax.shard_map(advance, mesh=mesh, in_specs=in_specs, out_specs=out_specs, check_vma=False)
```
